32 devices in a mesh: patch: 8 (over z, x), pair: 4 (over y, core).
Axes of the slice: x: 2, y: 2, z: 4, core: 2. Of those that a mesh axis runs over, the one named last changes fastest.
Arguments:
- node_latents: bfloat16 [8192, 1024], P('patch', 'pair'), may hold values from -12 to 12
- edge_latents: bfloat16 [16384, 1024], P('patch', 'pair'), may hold values from -12 to 12
- edge_sender: int32 [64, 256], P('patch'), may hold values from -1 to 2047, as said below
- edge_receiver: int32 [64, 256], P('patch'), may hold values from -1 to 255, as said below
- block_owner: int32 [64], P('patch'), may hold values from 0 to 7, as said below
- node_counts: int32 [8], P('patch'), may hold values from 512 to 1024, as said below
- halo_nodes: int32 [8, 8, 256], P('patch'), may hold values from 0 to 1023, as said below
- w_endpoints: bfloat16 [1024, 2, 1024], P(None, None, 'pair'), may hold values from -0.1875 to 0.1875
- w_edge_in: bfloat16 [1024, 1024], P(None, 'pair'), may hold values from -0.1875 to 0.1875
- edge_bias: float32 [1024], P('pair'), may hold values from -3 to 3
- w_edge_out: bfloat16 [1024, 1024], P('pair'), may hold values from -1 to 1
- edge_gain: float32 [1024], P('pair'), may hold values from 0.5 to 1.5
- edge_shift: float32 [1024], P('pair'), may hold values from -3 to 3
- w_node_in: bfloat16 [2, 1024, 1024], P(None, None, 'pair'), may hold values from -0.125 to 0.125
- node_bias: float32 [1024], P('pair'), may hold values from -3 to 3
- w_node_out: bfloat16 [1024, 1024], P('pair'), may hold values from -1 to 1
- node_gain: float32 [1024], P('pair'), may hold values from 0.5 to 1.5
- node_shift: float32 [1024], P('pair'), may hold values from -3 to 3
Outputs:
- updated_nodes: bfloat16 [8192, 1024], P('patch', 'pair')
- updated_edges: bfloat16 [16384, 1024], P('patch', 'pair')
The draws below stay inside these ranges and needn't reach their ends.
Inputs may be any that keep to these rules, and one draw needn't show every extreme that they name: `edge_sender`: section q = slot // 256 of a patch's halo table holds, in order, the nodes halo_nodes[q, that patch]; -1 stands exactly where edge_receiver is -1. `edge_receiver`: -1 marks padding and stands only after the live edges of a block; within a block the live values never fall and take at most 16 distinct values; every patch has a block with 256 live edges and 16 distinct receivers. `block_owner`: no patch owns more than 1 of the blocks of one patch; every patch owns 1 of its own blocks, and some patch owns 1 block of every patch. `node_counts`: some patch has 1024 live nodes. halo_nodes[q, d] lists local live nodes of patch q (below node_counts[q]); entries may repeat.
All inputs are finite; a program needn't handle non-finite values.
Results may differ from the reference program's by a relative error of at most 0.008.
Values may be sent and summed in bfloat16 or wider, within the bound.
No kernel may reach another device: no remote copies, remote signals or barrier semaphores. Data moves between devices by JAX's collectives and lax.ppermute only.
A program may use at most 128 MiB of HBM per device.

```python
import math
import jax
import jax.numpy as jnp
from jax import lax

D = 1024
TILE = 256
RT = 16
NODE_DEV = 1024
BLK_DEV = 8
CAP = 1
HALO = 256
HOT = 1
BLOCKS = 64
EDGES = 16384
NODES = 8192
N_PATCH = 8
N_PAIR = 4


def layout_ints(key):
    keys = jax.random.split(jax.random.fold_in(key, 101), 12)
    patch_ids = jnp.arange(N_PATCH, dtype=jnp.int32)
    hot_order = jnp.argsort(jax.random.randint(keys[0], (N_PATCH,), 0, 2 ** 20, dtype=jnp.int32) * N_PATCH + patch_ids)
    hot_rank = jnp.zeros((N_PATCH,), jnp.int32).at[hot_order].set(patch_ids)
    is_hot = (hot_rank < HOT).astype(jnp.int32)
    scores = jax.random.randint(keys[1], (N_PATCH, N_PATCH), 0, 2 ** 20, dtype=jnp.int32)
    scores = scores + is_hot[None, :] * 2 ** 21 + (patch_ids[:, None] == patch_ids[None, :]).astype(jnp.int32) * 2 ** 22
    scores = scores * N_PATCH + patch_ids[None, :]
    chosen = lax.top_k(scores, BLK_DEV // CAP)[1].astype(jnp.int32)
    chosen = jnp.repeat(chosen, CAP, axis=1)
    shuffle_score = jax.random.randint(keys[2], (N_PATCH, BLK_DEV), 0, 2 ** 20, dtype=jnp.int32) * BLK_DEV + jnp.arange(BLK_DEV, dtype=jnp.int32)[None, :]
    order = jnp.argsort(shuffle_score, axis=1)
    owners = jnp.take_along_axis(chosen, order, axis=1).reshape(BLOCKS).astype(jnp.int32)
    counts = jax.random.randint(keys[3], (N_PATCH,), NODE_DEV // 2, NODE_DEV + 1, dtype=jnp.int32)
    counts = jnp.where(is_hot > 0, NODE_DEV, counts).astype(jnp.int32)
    halo_lists = jax.random.randint(keys[4], (N_PATCH, N_PATCH, HALO), 0, counts[:, None, None], dtype=jnp.int32)
    block_ids = jnp.arange(BLOCKS, dtype=jnp.int32)
    live_count = jax.random.randint(keys[5], (BLOCKS,), TILE // 2, TILE + 1, dtype=jnp.int32)
    full_pick = jax.random.randint(keys[6], (N_PATCH,), 0, BLK_DEV, dtype=jnp.int32)
    live_count = jnp.where(block_ids % BLK_DEV == jnp.repeat(full_pick, BLK_DEV), TILE, live_count)
    fillers = jax.random.randint(keys[7], (BLOCKS, TILE - RT), 0, RT, dtype=jnp.int32)
    firsts = jnp.broadcast_to(jnp.arange(RT, dtype=jnp.int32)[None, :], (BLOCKS, RT))
    segment = jnp.sort(jnp.concatenate([firsts, fillers], axis=1), axis=1)
    slot_score = jax.random.randint(keys[8], (BLOCKS, HALO), 0, 2 ** 20, dtype=jnp.int32) * HALO + jnp.arange(HALO, dtype=jnp.int32)[None, :]
    slot_list = jnp.sort(jnp.argsort(slot_score, axis=1)[:, :RT].astype(jnp.int32), axis=1)
    positions = jnp.arange(TILE, dtype=jnp.int32)[None, :]
    is_live = positions < live_count[:, None]
    receiver = jnp.where(is_live, jnp.take_along_axis(slot_list, segment, axis=1), -1).astype(jnp.int32)
    coin = jax.random.randint(keys[9], (BLOCKS, TILE), 0, 2, dtype=jnp.int32)
    other = jax.random.randint(keys[10], (BLOCKS, TILE), 0, N_PATCH, dtype=jnp.int32)
    section = jnp.where(coin > 0, owners[:, None], other)
    within = jax.random.randint(keys[11], (BLOCKS, TILE), 0, HALO, dtype=jnp.int32)
    sender = jnp.where(is_live, section * HALO + within, -1).astype(jnp.int32)
    return (owners, counts, halo_lists, sender, receiver)


def draw_edge_sender(key, part):
    return layout_ints(key)[3]


def draw_edge_receiver(key, part):
    return layout_ints(key)[4]


def draw_block_owner(key, part):
    return layout_ints(key)[0]


def draw_node_counts(key, part):
    return layout_ints(key)[1]


def draw_halo_nodes(key, part):
    return layout_ints(key)[2]


def scaled_rows(key, rows_count, cols_count):
    key_base, key_scale = jax.random.split(jax.random.fold_in(key, 5), 2)
    base = jax.random.normal(key_base, (rows_count, cols_count), jnp.float32)
    scale = jnp.exp(jax.random.uniform(key_scale, (rows_count, 1), jnp.float32, math.log(0.3), math.log(3.0)))
    value = base * scale
    return jnp.clip(value, -12.0, 12.0)


def draw_node_latents(key, part):
    return scaled_rows(key, NODES, D).astype(jnp.bfloat16)


def draw_edge_latents(key, part):
    return scaled_rows(key, EDGES, D).astype(jnp.bfloat16)


def rising_columns(key):
    key_base, key_jitter = jax.random.split(jax.random.fold_in(key, 9), 2)
    base = jax.random.normal(key_base, (D, D), jnp.float32) / math.sqrt(D)
    ramp = (jnp.arange(D, dtype=jnp.float32) / (D - 1))[None, :]
    scale = jnp.exp(math.log(0.5) + ramp * math.log(10.0)) * jax.random.uniform(key_jitter, (1, D), jnp.float32, 0.7, 1.3)
    return jnp.clip(base * scale, -1.0, 1.0).astype(jnp.bfloat16)


def draw_w_edge_out(key, part):
    return rising_columns(key)


def draw_w_node_out(key, part):
    return rising_columns(jax.random.fold_in(key, 3))


def block_scale(rng, extent, pieces, low, high):
    level = 1.0
    for axis_at, parts in pieces:
        draws = jax.random.uniform(jax.random.fold_in(jax.random.fold_in(rng, 6), axis_at), (parts,), jnp.float32, low / len(pieces), high / len(pieces))
        level = level * jnp.repeat(jnp.exp(draws), extent[axis_at] // parts).reshape((-1,) + (1,) * (len(extent) - 1 - axis_at))
    return level


def scatter_about(rng, dims, deviation, reach, cuts=(), kind=jnp.bfloat16):
    values = deviation * jax.random.normal(rng, dims, jnp.float32)
    if cuts:
        values = values * block_scale(rng, dims, cuts, -0.22, 0.18)
    return jnp.clip(values, -reach, reach).astype(kind)


def setup_inputs(seed: int = 0) -> dict:
    key_of = jax.random.split(jax.random.key(seed), 19)
    return {
        "node_latents": draw_node_latents(jax.random.fold_in(key_of[18], 71), 0),
        "edge_latents": draw_edge_latents(jax.random.fold_in(key_of[18], 71), 0),
        "edge_sender": draw_edge_sender(jax.random.fold_in(key_of[18], 71), 0),
        "edge_receiver": draw_edge_receiver(jax.random.fold_in(key_of[18], 71), 0),
        "block_owner": draw_block_owner(jax.random.fold_in(key_of[18], 71), 0),
        "node_counts": draw_node_counts(jax.random.fold_in(key_of[18], 71), 0),
        "halo_nodes": draw_halo_nodes(jax.random.fold_in(key_of[18], 71), 0),
        "w_endpoints": scatter_about(key_of[7], (D, 2, D), D ** -0.5, 0.1875, ((2, 4),)),
        "w_edge_in": scatter_about(key_of[8], (D, D), D ** -0.5, 0.1875, ((1, 4),)),
        "edge_bias": scatter_about(key_of[9], (D,), 0.5, 3.0, ((0, 4),), jnp.float32),
        "w_edge_out": draw_w_edge_out(jax.random.fold_in(key_of[18], 71), 0),
        "edge_gain": jnp.clip(1.0 + 0.1 * jax.random.normal(key_of[11], (D,), jnp.float32), 0.5, 1.5),
        "edge_shift": scatter_about(key_of[12], (D,), 0.5, 3.0, ((0, 4),), jnp.float32),
        "w_node_in": scatter_about(key_of[13], (2, D, D), (2 * D) ** -0.5, 0.125, ((2, 4),)),
        "node_bias": scatter_about(key_of[14], (D,), 0.5, 3.0, ((0, 4),), jnp.float32),
        "w_node_out": draw_w_node_out(jax.random.fold_in(key_of[18], 71), 0),
        "node_gain": jnp.clip(1.0 + 0.1 * jax.random.normal(key_of[16], (D,), jnp.float32), 0.5, 1.5),
        "node_shift": scatter_about(key_of[17], (D,), 0.5, 3.0, ((0, 4),), jnp.float32),
    }


EPS = 1e-05

def pair_sum(hidden, weight):
    rows_count = hidden.shape[0]
    share = weight.shape[0] // N_PAIR
    total_sum = jnp.zeros((rows_count, weight.shape[1]), jnp.float32)
    for member in range(N_PAIR):
        term = jnp.dot(hidden[:, member * share:(member + 1) * share], weight[member * share:(member + 1) * share], preferred_element_type=jnp.float32)
        rounded = lax.optimization_barrier(term.astype(jnp.bfloat16))
        total_sum = total_sum + rounded.astype(jnp.float32)
    return total_sum

def normalize(values, gain_row, shift_row):
    row_mean = lax.optimization_barrier(jnp.mean(values, axis=1, keepdims=True))
    square = lax.optimization_barrier(jnp.mean(values * values, axis=1, keepdims=True))
    return (values - row_mean) * lax.rsqrt(square - row_mean * row_mean + EPS) * gain_row[None, :] + shift_row[None, :]

def reference(node_latents, edge_latents, edge_sender, edge_receiver, block_owner, node_counts, halo_nodes, w_endpoints, w_edge_in, edge_bias, w_edge_out, edge_gain, edge_shift, w_node_in, node_bias, w_node_out, node_gain, node_shift):
    projected = jnp.dot(node_latents, w_endpoints.reshape(D, 2 * D), preferred_element_type=jnp.float32).astype(jnp.bfloat16).reshape(NODES, 2, D)
    device_edges = BLK_DEV * TILE

    def one_device(aggregate, device):
        rows_in = lax.dynamic_slice_in_dim(edge_latents, (device * device_edges).astype(jnp.int32), device_edges, 0)
        senders = lax.dynamic_slice_in_dim(edge_sender, (device * BLK_DEV).astype(jnp.int32), BLK_DEV, 0).reshape(-1)
        receivers = lax.dynamic_slice_in_dim(edge_receiver, (device * BLK_DEV).astype(jnp.int32), BLK_DEV, 0).reshape(-1)
        owners = lax.dynamic_slice_in_dim(block_owner, (device * BLK_DEV).astype(jnp.int32), BLK_DEV, 0)
        edge_owner = jnp.repeat(owners, TILE)
        is_live = receivers >= 0
        sender_clip = jnp.maximum(senders, 0)
        sender_patch = sender_clip // HALO
        sender_node = sender_patch * NODE_DEV + halo_nodes[sender_patch, device, sender_clip - sender_patch * HALO]
        receiver_node = edge_owner * NODE_DEV + halo_nodes[edge_owner, device, jnp.maximum(receivers, 0)]
        edge_pre = jnp.dot(rows_in, w_edge_in, preferred_element_type=jnp.float32)
        edge_pre = edge_pre + projected[sender_node, 0].astype(jnp.float32) + projected[receiver_node, 1].astype(jnp.float32) + edge_bias[None, :]
        edge_hidden = jax.nn.silu(edge_pre).astype(jnp.bfloat16)
        edge_mixed = pair_sum(edge_hidden, w_edge_out)
        edge_norm = normalize(edge_mixed, edge_gain, edge_shift)
        old_rows = rows_in.astype(jnp.float32)
        new_rows = jnp.where(is_live[:, None], old_rows + edge_norm, old_rows).astype(jnp.bfloat16)
        target = jnp.where(is_live, receiver_node, NODES).astype(jnp.int32)
        aggregate = aggregate.at[target].add(new_rows.astype(jnp.float32))
        return (aggregate, new_rows)
    aggregate, new_edges = lax.scan(one_device, jnp.zeros((NODES + 1, D), jnp.float32), jnp.arange(N_PATCH, dtype=jnp.int32))
    aggregated = aggregate[:NODES].astype(jnp.bfloat16)
    node_pre = jnp.dot(node_latents, w_node_in[0], preferred_element_type=jnp.float32)
    node_pre = node_pre + jnp.dot(aggregated, w_node_in[1], preferred_element_type=jnp.float32) + node_bias[None, :]
    node_hidden = jax.nn.silu(node_pre).astype(jnp.bfloat16)
    node_mixed = pair_sum(node_hidden, w_node_out)
    node_norm = normalize(node_mixed, node_gain, node_shift)
    live_nodes = jnp.arange(NODES, dtype=jnp.int32) % NODE_DEV < jnp.repeat(node_counts, NODE_DEV)
    old_nodes = node_latents.astype(jnp.float32)
    updated_nodes = jnp.where(live_nodes[:, None], old_nodes + node_norm, old_nodes).astype(jnp.bfloat16)
    return (updated_nodes, new_edges.reshape(EDGES, D))
```

```python
import functools

import jax
import jax.numpy as jnp
from jax import lax
from jax.experimental import pallas as pl
from jax.experimental.pallas import tpu as pltpu
from jax.sharding import PartitionSpec as P

RT = 16
EPS = 1e-05


BF = jnp.bfloat16
F32 = jnp.float32
VMEM = pl.BlockSpec(memory_space=pltpu.VMEM)
SMEM = pl.BlockSpec(memory_space=pltpu.SMEM)


def swap(value, axis, mask):
    size = lax.axis_size(axis)
    return lax.ppermute(value, axis, [(i, i ^ mask) for i in range(size)])


def pick_kernel(count, index_ref, *refs):
    tables, out_ref = refs[:count], refs[count]
    index = index_ref[...]
    total = None
    start = 0
    for table in tables:
        rows = table.shape[0]
        slots = lax.broadcasted_iota(jnp.int32, (index.shape[0], rows), 1) + start
        hot = (index == slots).astype(F32).astype(BF)
        part = jnp.dot(hot, table[...], preferred_element_type=F32)
        total = part if total is None else total + part
        start += rows
    out_ref[...] = total.astype(out_ref.dtype)


def pick_rows(index, tables, tiles):
    rows, width = index.shape[0], tables[0].shape[1]
    tile = rows // tiles
    depth = sum(t.shape[0] for t in tables)
    return pl.pallas_call(
        functools.partial(pick_kernel, len(tables)),
        grid=(tiles,),
        in_specs=[pl.BlockSpec((tile, 1), lambda i: (i, 0))]
        + [pl.BlockSpec(t.shape, lambda i: (0, 0)) for t in tables],
        out_specs=pl.BlockSpec((tile, width), lambda i: (i, 0)),
        out_shape=jax.ShapeDtypeStruct((rows, width), tables[0].dtype),
        cost_estimate=pl.CostEstimate(
            flops=2 * rows * depth * width,
            bytes_accessed=2 * (rows + depth) * width,
            transcendentals=0,
        ),
    )(index, *tables)


def silu(value):
    return value / (1.0 + jnp.exp(-value))


def finish(mixed, old, gain, shift, live):
    width = mixed.shape[1]
    mean = jnp.sum(mixed, axis=1, keepdims=True) / width
    square = jnp.sum(mixed * mixed, axis=1, keepdims=True) / width
    norm = (mixed - mean) * lax.rsqrt(square - mean * mean + EPS) * gain + shift
    return jnp.where(live, old + norm, old).astype(BF)


def edge_kernel(pairs, groups, me_ref, segment_ref, segrow_ref, bias_ref, gain_ref, shift_ref, *refs):
    e_refs, refs = refs[:pairs], refs[pairs:]
    s_refs, refs = refs[:pairs], refs[pairs:]
    a_refs, refs = refs[:pairs], refs[pairs:]
    b_refs, refs = refs[:pairs], refs[pairs:]
    out_ref, sums_ref, e_all, s_all, r_all = refs
    me = me_ref[0]
    rows, local = e_refs[0].shape
    full = local * pairs
    tile = rows // groups
    slots = s_refs[0].shape[0] - rows
    per = slots // groups
    for k in range(pairs):
        at = pl.ds(pl.multiple_of((me ^ k) * local, local), local)
        e_all[:, at] = e_refs[k][...]
        s_all[:, at] = s_refs[k][...]
    for k in range(pairs):
        r_all[:, k * local : (k + 1) * local] = jnp.dot(
            s_all[rows:, :], a_refs[k][2 * full :, :], preferred_element_type=F32
        ).astype(BF)

    def block(g, _):
        base = pl.multiple_of(g * tile, tile)
        segment = segment_ref[pl.ds(base, tile), :]
        hot = (segment == lax.broadcasted_iota(jnp.int32, (tile, slots), 1) - g * per)
        hot = (hot & (segment < per)).astype(F32).astype(BF)
        edges = e_all[pl.ds(base, tile), :]
        senders = s_all[pl.ds(base, tile), :]
        mixed = None
        for k in range(pairs):
            pre = jnp.dot(edges, a_refs[k][:full, :], preferred_element_type=F32)
            pre += jnp.dot(senders, a_refs[k][full : 2 * full, :], preferred_element_type=F32).astype(BF).astype(F32)
            pre += jnp.dot(hot, r_all[:, k * local : (k + 1) * local], preferred_element_type=F32)
            pre += bias_ref[pl.ds(me ^ k, 1), :]
            hidden = silu(pre).astype(BF)
            part = jnp.dot(hidden, b_refs[k][...], preferred_element_type=F32).astype(BF).astype(F32)
            mixed = part if mixed is None else mixed + part
        live = segment < per
        new = finish(mixed, edges.astype(F32), gain_ref[...], shift_ref[...], live)
        e_all[pl.ds(base, tile), :] = new
        segrow = segrow_ref[pl.ds(g, 1), :]
        member = (segrow == lax.broadcasted_iota(jnp.int32, (per, tile), 0)).astype(F32).astype(BF)
        total = jnp.dot(member, new, preferred_element_type=F32)
        sums_ref[pl.ds(pl.multiple_of(g * per, per), per), :] = total.astype(BF)
        return 0

    lax.fori_loop(0, groups, block, 0)
    for k in range(pairs):
        at = pl.ds(pl.multiple_of((me ^ k) * local, local), local)
        out_ref[k] = e_all[:, at]


def node_kernel(pairs, sources, me_ref, count_ref, ids_ref, bias_ref, gain_ref, shift_ref, *refs):
    n_refs, refs = refs[:pairs], refs[pairs:]
    r_refs, refs = refs[:sources], refs[sources:]
    c_refs, refs = refs[:pairs], refs[pairs:]
    d_refs, refs = refs[:pairs], refs[pairs:]
    out_ref, n_all = refs
    me = me_ref[0]
    rows, local = n_refs[0].shape
    full = local * pairs
    first = me * rows
    for k in range(pairs):
        at = pl.ds(pl.multiple_of((me ^ k) * local, local), local)
        n_all[:, at] = n_refs[k][...]
    nodes = n_all[...]
    total = None
    start = 0
    for r in r_refs:
        depth = r.shape[0]
        ids = ids_ref[:, start : start + depth]
        hot = ids == lax.broadcasted_iota(jnp.int32, (rows, depth), 0) + first
        part = jnp.dot(hot.astype(F32).astype(BF), r[...], preferred_element_type=F32)
        total = part if total is None else total + part
        start += depth
    aggregated = total.astype(BF)
    mixed = None
    for k in range(pairs):
        pre = jnp.dot(nodes, c_refs[k][:full, :], preferred_element_type=F32)
        pre += jnp.dot(aggregated, c_refs[k][full:, :], preferred_element_type=F32)
        pre += bias_ref[pl.ds(me ^ k, 1), :]
        hidden = silu(pre).astype(BF)
        part = jnp.dot(hidden, d_refs[k][...], preferred_element_type=F32).astype(BF).astype(F32)
        mixed = part if mixed is None else mixed + part
    live = lax.broadcasted_iota(jnp.int32, (rows, 1), 0) + first < count_ref[0]
    n_all[...] = finish(mixed, nodes.astype(F32), gain_ref[...], shift_ref[...], live)
    for k in range(pairs):
        at = pl.ds(pl.multiple_of((me ^ k) * local, local), local)
        out_ref[k] = n_all[:, at]


def shards(
    node_latents,
    edge_latents,
    edge_sender,
    edge_receiver,
    block_owner,
    node_counts,
    halo_nodes,
    w_endpoints,
    w_edge_in,
    edge_bias,
    w_edge_out,
    edge_gain,
    edge_shift,
    w_node_in,
    node_bias,
    w_node_out,
    node_gain,
    node_shift,
):
    patches = lax.axis_size("patch")
    pairs = lax.axis_size("pair")
    patch = lax.axis_index("patch")
    me = lax.axis_index("pair")
    full, local = w_edge_in.shape
    node_total = node_latents.shape[0]
    edge_total = edge_latents.shape[0]
    blocks, tile = edge_sender.shape
    halo = halo_nodes.shape[2]
    mine = blocks // pairs
    rows = edge_total // pairs
    quarter = node_total // pairs
    peers = jnp.arange(pairs, dtype=jnp.int32) ^ me
    by_swap = patches <= 8
    order = jnp.arange(patches, dtype=jnp.int32)
    order = order ^ patch if by_swap else order

    def to_patches(pieces):
        if by_swap:
            return [pieces[0]] + [swap(pieces[k], "patch", k) for k in range(1, patches)]
        return list(lax.all_to_all(jnp.stack(pieces), "patch", 0, 0, tiled=True))

    def to_pairs(pieces):
        return [pieces[0]] + [swap(pieces[k], "pair", k) for k in range(1, pairs)]

    send_list = halo_nodes[0][order]
    picked = pick_rows(send_list.reshape(-1, 1), [node_latents], 4)
    picked = picked.reshape(patches, halo, local)
    table = to_patches([picked[k] for k in range(patches)])

    previous = jnp.concatenate([jnp.full((blocks, 1), -2, jnp.int32), edge_receiver[:, :-1]], axis=1)
    segment = jnp.cumsum((edge_receiver != previous).astype(jnp.int32), axis=1) - 1
    segment = jnp.where(edge_receiver >= 0, segment, RT)
    member = segment[:, None, :] == jnp.arange(RT, dtype=jnp.int32)[None, :, None]
    tile_ids = jnp.max(jnp.where(member, edge_receiver[:, None, :], -1), axis=2)

    def place(owner):
        return (owner ^ patch if by_swap else owner) * halo

    sender_at = place(edge_sender // halo) + edge_sender % halo
    sender_at = jnp.where(edge_sender >= 0, sender_at, 0).reshape(pairs, rows)
    receiver_at = place(block_owner)[:, None] + jnp.maximum(tile_ids, 0)
    wanted = jnp.concatenate([sender_at, receiver_at.reshape(pairs, mine * RT)], axis=1)
    wanted = wanted[peers].reshape(-1, 1)
    chosen = (block_owner[None, :] == order[:, None])
    send_ids = jnp.max(jnp.where(chosen[:, :, None], tile_ids[None], -1), axis=1)
    got_ids = to_patches([send_ids[k] for k in range(patches)])
    got_ids = jnp.stack(got_ids)
    node_ids = jnp.take_along_axis(send_list, jnp.maximum(got_ids, 0), axis=1)
    node_ids = jnp.where(got_ids >= 0, node_ids, -1).reshape(1, -1)

    def gather_slices(weight):
        size = weight.shape[0] // 2
        odd = patch % 2
        pieces = {0: weight}
        mask = pairs // 2
        first = True
        while mask:
            for k in sorted(pieces):
                if first and patches % 2 == 0:
                    half = lax.dynamic_slice_in_dim(pieces[k], odd * size, size, 0)
                    near = swap(half, "pair", mask)
                    other = swap(near, "patch", 1)
                    low = jnp.where(odd == 0, near, other)
                    high = jnp.where(odd == 0, other, near)
                    pieces[k ^ mask] = jnp.concatenate([low, high], axis=0)
                else:
                    pieces[k ^ mask] = swap(pieces[k], "pair", mask)
            first = False
            mask //= 2
        return [pieces[k] for k in range(pairs)]

    ends = jnp.concatenate([w_edge_in, w_endpoints[:, 0], w_endpoints[:, 1]], axis=0)
    a_parts = gather_slices(ends)
    b_parts = gather_slices(w_edge_out)
    vectors = jnp.stack([edge_bias, edge_gain, edge_shift, node_bias, node_gain, node_shift])
    vectors = lax.all_gather(vectors, "pair", axis=0, tiled=False)
    e_bias, e_gain, e_shift, n_bias, n_gain, n_shift = (vectors[:, i] for i in range(6))

    own_edges = edge_latents.reshape(pairs, rows, local)
    e_parts = to_pairs([lax.dynamic_index_in_dim(own_edges, me ^ k, 0, False) for k in range(pairs)])
    seen = pick_rows(wanted, table, pairs).reshape(pairs, rows + mine * RT, local)
    s_parts = to_pairs([seen[k] for k in range(pairs)])

    my_segment = lax.dynamic_slice_in_dim(segment, me * mine, mine, 0)
    me_scalar = me.reshape(1).astype(jnp.int32)
    new_edges, sums = pl.pallas_call(
        functools.partial(edge_kernel, pairs, mine),
        in_specs=[SMEM] + [VMEM] * (5 + 4 * pairs),
        out_specs=[VMEM, VMEM],
        out_shape=[
            jax.ShapeDtypeStruct((pairs, rows, local), BF),
            jax.ShapeDtypeStruct((mine * RT, full), BF),
        ],
        scratch_shapes=[
            pltpu.VMEM((rows, full), BF),
            pltpu.VMEM((rows + mine * RT, full), BF),
            pltpu.VMEM((mine * RT, full), BF),
        ],
        cost_estimate=pl.CostEstimate(
            flops=6 * rows * full * full, bytes_accessed=10 * full * full, transcendentals=rows * full
        ),
    )(
        me_scalar,
        my_segment.reshape(-1, 1),
        my_segment,
        e_bias,
        e_gain.reshape(1, full),
        e_shift.reshape(1, full),
        *e_parts,
        *s_parts,
        *a_parts,
        *b_parts,
    )

    def unsplit(pieces):
        depth = pieces[0].shape[0]
        total = jnp.zeros((depth * pairs, local), BF)
        for k in range(pairs):
            total = lax.dynamic_update_slice_in_dim(total, pieces[k], (me ^ k) * depth, 0)
        return total

    all_sums = jnp.stack(to_pairs([sums] * pairs)).reshape(blocks, RT * full)
    owners = block_owner.reshape(pairs, mine)[peers].reshape(-1)
    take = (owners[None, :] == order[:, None]).astype(BF)
    sent = jnp.dot(take, all_sums, preferred_element_type=F32).astype(BF).reshape(patches, RT, full)
    got = to_patches([sent[k] for k in range(patches)])

    edges_out = unsplit(to_pairs([new_edges[k] for k in range(pairs)]))

    c_parts = gather_slices(w_node_in.reshape(2 * full, local))
    d_parts = gather_slices(w_node_out)
    own_nodes = node_latents.reshape(pairs, quarter, local)
    n_parts = to_pairs([lax.dynamic_index_in_dim(own_nodes, me ^ k, 0, False) for k in range(pairs)])
    new_nodes = pl.pallas_call(
        functools.partial(node_kernel, pairs, len(got)),
        in_specs=[SMEM, SMEM] + [VMEM] * (4 + 3 * pairs + len(got)),
        out_specs=VMEM,
        out_shape=jax.ShapeDtypeStruct((pairs, quarter, local), BF),
        scratch_shapes=[pltpu.VMEM((quarter, full), BF)],
        cost_estimate=pl.CostEstimate(
            flops=6 * quarter * full * full, bytes_accessed=8 * full * full, transcendentals=quarter * full
        ),
    )(
        me_scalar,
        node_counts,
        node_ids,
        n_bias,
        n_gain.reshape(1, full),
        n_shift.reshape(1, full),
        *n_parts,
        *got,
        *c_parts,
        *d_parts,
    )
    nodes_out = unsplit(to_pairs([new_nodes[k] for k in range(pairs)]))
    return (nodes_out, edges_out)


def solution(mesh):
    return jax.shard_map(
        shards,
        mesh=mesh,
        in_specs=(
            P("patch", "pair"),
            P("patch", "pair"),
            P("patch", None),
            P("patch", None),
            P("patch"),
            P("patch"),
            P("patch", None, None),
            P(None, None, "pair"),
            P(None, "pair"),
            P("pair"),
            P("pair", None),
            P("pair"),
            P("pair"),
            P(None, None, "pair"),
            P("pair"),
            P("pair", None),
            P("pair"),
            P("pair"),
        ),
        out_specs=(P("patch", "pair"), P("patch", "pair")),
        check_vma=False,
    )
```

```python
import functools

import jax
import jax.numpy as jnp
from jax import lax
from jax.experimental import pallas as pl
from jax.experimental.pallas import tpu as pltpu
from jax.sharding import PartitionSpec as P

RT = 16
EPS = 1e-05
LANES = 128
TAIL = 16


BF = jnp.bfloat16
F32 = jnp.float32
VMEM = pl.BlockSpec(memory_space=pltpu.VMEM)
SMEM = pl.BlockSpec(memory_space=pltpu.SMEM)
ANY = pl.BlockSpec(memory_space=pl.ANY)


def swap(value, axis, mask):
    size = lax.axis_size(axis)
    return lax.ppermute(value, axis, [(i, i ^ mask) for i in range(size)])


def column(row):
    wide = jnp.broadcast_to(row.astype(F32), (LANES, row.shape[1]))
    return jnp.transpose(wide).astype(jnp.int32)


def hot_lanes(index, start, count):
    parts = []
    for at in range(0, count, LANES):
        width = min(LANES, count - at)
        lane = lax.broadcasted_iota(jnp.int32, (index.shape[0], width), 1) + (start + at)
        parts.append(jnp.where(index[:, :width] == lane, 1.0, 0.0).astype(BF))
    return parts[0] if len(parts) == 1 else jnp.concatenate(parts, axis=1)


def pick_kernel(count, groups, order_ref, index_ref, *refs):
    tables, outs = refs[:count], refs[count:]
    rows = outs[0].shape[0]
    for g in range(groups):
        index = column(index_ref[pl.ds(order_ref[g], 1), :])[:rows]
        total = None
        start = 0
        for table in tables:
            hot = hot_lanes(index, start, table.shape[0])
            part = jnp.dot(hot, table[...], preferred_element_type=F32)
            total = part if total is None else total + part
            start += table.shape[0]
        outs[g][...] = total.astype(BF)


def pick_rows(order, index, tables, rows):
    groups, width = index.shape[0], tables[0].shape[1]
    depth = sum(t.shape[0] for t in tables)
    return pl.pallas_call(
        functools.partial(pick_kernel, len(tables), groups),
        in_specs=[SMEM] + [VMEM] * (1 + len(tables)),
        out_specs=[VMEM] * groups,
        out_shape=[jax.ShapeDtypeStruct((rows, width), BF)] * groups,
        cost_estimate=pl.CostEstimate(
            flops=2 * groups * rows * depth * width,
            bytes_accessed=2 * (groups * rows + depth) * width,
            transcendentals=0,
        ),
    )(order, index, *tables)


def split_kernel(size, per, order_ref, in_ref, vectors_ref, *outs):
    value = vectors_ref[...]
    high = value.astype(BF).astype(F32)
    middle = (value - high).astype(BF).astype(F32)
    low = value - high - middle
    parts = [high, middle, low]
    parts.append(jnp.zeros((TAIL - 3 * value.shape[0], value.shape[1]), F32))
    tail = jnp.concatenate(parts, axis=0).astype(BF)
    for k, out in enumerate(outs):
        for i in range(per):
            at = pl.multiple_of(order_ref[k * per + i] * size, size)
            out[i * size : (i + 1) * size, :] = in_ref[pl.ds(at, size), :]
        out[per * size :, :] = tail


def unpack_vectors(tail, count):
    wide = tail.astype(F32)
    return wide[:count] + wide[count : 2 * count] + wide[2 * count : 3 * count]


def join_kernel(size, per, order_ref, *refs):
    out = refs[-1]
    for k, part in enumerate(refs[:-1]):
        for i in range(per):
            at = pl.multiple_of(order_ref[k * per + i] * size, size)
            out[pl.ds(at, size), :] = part[i * size : (i + 1) * size, :]


def split(order, size, per, value, vectors):
    parts = order.shape[0] // per
    return pl.pallas_call(
        functools.partial(split_kernel, size, per),
        in_specs=[SMEM, VMEM, VMEM],
        out_specs=[VMEM] * parts,
        out_shape=[jax.ShapeDtypeStruct((size * per + TAIL, value.shape[1]), BF)] * parts,
    )(order, value, vectors)


def pack_edge_kernel(flags_ref, in_ref, ends_ref, out_ref, packed, *pieces):
    odd = flags_ref[0]
    full, local = in_ref.shape
    packed[:full, :] = in_ref[...]
    step = 2 * LANES
    for side in range(2):
        lane = lax.broadcasted_iota(jnp.int32, (LANES, step), 1)
        row = lax.broadcasted_iota(jnp.int32, (LANES, step), 0)
        hot = jnp.where(lane == 2 * row + side, 1.0, 0.0).astype(BF)
        for n in range(full // LANES):
            part = jnp.dot(hot, ends_ref[n * step : (n + 1) * step, :], preferred_element_type=F32)
            base = (1 + side) * full + n * LANES
            packed[base : base + LANES, :] = part.astype(BF)
    for c in range(full // local):
        base = 3 * full + c * local
        packed[base : base + local, :] = out_ref[:, c * local : (c + 1) * local]
    copy_pieces(odd, packed, pieces)


def pack_node_kernel(flags_ref, in_ref, out_ref, packed, *pieces):
    odd = flags_ref[0]
    rows, local = in_ref.shape
    packed[:rows, :] = in_ref[...]
    for c in range(out_ref.shape[1] // local):
        base = rows + c * local
        packed[base : base + local, :] = out_ref[:, c * local : (c + 1) * local]
    copy_pieces(odd, packed, pieces)


def copy_pieces(odd, packed, pieces):
    start = 0
    for piece in pieces:
        half = piece.shape[0]
        piece[...] = packed[pl.ds(pl.multiple_of(start + odd * half, half), half), :]
        start += 2 * half


def pack(kernel, flags, chunks, *weights):
    total = sum(size for _, size in chunks)
    local = weights[0].shape[1]
    return pl.pallas_call(
        kernel,
        in_specs=[SMEM] + [VMEM] * len(weights),
        out_specs=[VMEM] * (1 + len(chunks)),
        out_shape=[jax.ShapeDtypeStruct((total, local), BF)]
        + [jax.ShapeDtypeStruct((size // 2, local), BF) for _, size in chunks],
    )(flags, *weights)


def join(order, size, per, values):
    return pl.pallas_call(
        functools.partial(join_kernel, size, per),
        in_specs=[SMEM] + [VMEM] * len(values),
        out_specs=VMEM,
        out_shape=jax.ShapeDtypeStruct((size * order.shape[0], values[0].shape[1]), BF),
    )(order, *values)


def silu(value):
    return value / (1.0 + jnp.exp(-value))


def finish(mixed, old, gain, shift, live):
    width = mixed.shape[1]
    mean = jnp.sum(mixed, axis=1, keepdims=True) / width
    square = jnp.sum(mixed * mixed, axis=1, keepdims=True) / width
    norm = (mixed - mean) * lax.rsqrt(square - mean * mean + EPS) * gain + shift
    return jnp.where(live, old + norm, old).astype(BF)


def weight_copies(odd, chunks, refs, store, sems):
    own, near, far = refs[0], refs[1], refs[2:]
    copies = [
        [pltpu.make_async_copy(own, store.at[0], sems.at[0])],
        [pltpu.make_async_copy(near, store.at[1], sems.at[1])],
    ]
    at = 2
    for k in (2, 3):
        mine = []
        for start, size in chunks:
            for slot in (odd, 1 - odd):
                half = size // 2
                row = pl.multiple_of(start + slot * half, half)
                mine.append(pltpu.make_async_copy(far[at - 2], store.at[k, pl.ds(row, half)], sems.at[at]))
                at += 1
        copies.append(mine)
    return copies


def edge_kernel(pairs, groups, chunks, flags_ref, segrow_ref, ids_ref, *refs):
    e_refs, refs = refs[:pairs], refs[pairs:]
    s_refs, refs = refs[:pairs], refs[pairs:]
    count = 2 + 4 * len(chunks)
    w_refs, refs = refs[:count], refs[count:]
    outs, refs = refs[:pairs], refs[pairs:]
    sum_refs, refs = refs[:groups], refs[groups:]
    both, r_all, hidden, new_all, wide, store, sems = refs
    me, odd, turn = flags_ref[0], flags_ref[1], flags_ref[2]
    copies = weight_copies(odd, chunks, w_refs, store, sems)
    for group in copies:
        for copy in group:
            copy.start()
    rows, full = new_all.shape
    local = full // pairs
    tile = rows // groups
    bias = []
    for k in range(pairs):
        at = pl.multiple_of((me ^ k) * local, local)
        both[:, pl.ds(at, local)] = e_refs[k][:rows, :]
        both[:, pl.ds(at + full, local)] = s_refs[k][:rows, :]
        r_all[:, pl.ds(at, local)] = s_refs[k][rows:, :]
        vectors = unpack_vectors(e_refs[k][rows:, :], 3)
        bias.append(vectors[:1])
        wide[:1, pl.ds(at, local)] = vectors[1:2]
        wide[1:2, pl.ds(at, local)] = vectors[2:3]
    segments, hots = [], []
    for g in range(groups):
        segment = column(segrow_ref[g : g + 1, :])
        segments.append(segment)
        hots.append(hot_lanes(segment, 0, RT))
    for k in range(pairs):
        for copy in copies[k]:
            copy.wait()
        receivers = jnp.dot(r_all[...], store[k, 2 * full : 3 * full, :], preferred_element_type=F32).astype(BF)
        for g in range(groups):
            at = slice(g * tile, (g + 1) * tile)
            pre = jnp.dot(both[at, :], store[k, : 2 * full, :], preferred_element_type=F32)
            pre += jnp.dot(hots[g], receivers[g * RT : (g + 1) * RT], preferred_element_type=F32)
            hidden[at, k * local : (k + 1) * local] = silu(pre + bias[k]).astype(BF)
    for g in range(groups):
        at = slice(g * tile, (g + 1) * tile)
        mixed = []
        for c in range(pairs):
            base = 3 * full + c * local
            total = None
            for k in range(pairs):
                part = jnp.dot(
                    hidden[at, k * local : (k + 1) * local],
                    store[k, base : base + local, :],
                    preferred_element_type=F32,
                )
                total = part if total is None else total + part
            mixed.append(total)
        mixed = jnp.concatenate(mixed, axis=1)
        live = segments[g][:, :1] < RT
        old = both[at, :full].astype(F32)
        new_all[at, :] = finish(mixed, old, wide[:1, :], wide[1:2, :], live)
    for t in range(groups):
        g = t ^ turn
        segrow = segrow_ref[pl.ds(g, 1), :]
        member = segrow == lax.broadcasted_iota(jnp.int32, (RT, tile), 0)
        member = jnp.where(member, 1.0, 0.0).astype(BF)
        new = new_all[pl.ds(pl.multiple_of(g * tile, tile), tile), :]
        total = jnp.dot(member, new, preferred_element_type=F32)
        sum_refs[t][:, :full] = total.astype(BF)
        sum_refs[t][:, full:] = ids_ref[pl.ds(pl.multiple_of(g * RT, RT), RT), :]
    for k in range(pairs):
        at = pl.ds(pl.multiple_of((me ^ k) * local, local), local)
        outs[k][...] = new_all[:, at]


def node_kernel(pairs, sources, chunks, flags_ref, count_ref, from_ref, list_ref, *refs):
    n_refs, refs = refs[:pairs], refs[pairs:]
    r_refs, refs = refs[:sources], refs[sources:]
    count = 2 + 4 * len(chunks)
    w_refs, refs = refs[:count], refs[count:]
    outs, refs = refs[:pairs], refs[pairs:]
    n_all, sums, nodes_of, wide, store, sems = refs
    me, odd = flags_ref[0], flags_ref[1]
    copies = weight_copies(odd, chunks, w_refs, store, sems)
    for group in copies:
        for copy in group:
            copy.start()
    rows, full = n_all.shape
    local = full // pairs
    first = me * rows
    bias = []
    for k in range(pairs):
        at = pl.ds(pl.multiple_of((me ^ k) * local, local), local)
        n_all[:, at] = n_refs[k][:rows, :]
        vectors = unpack_vectors(n_refs[k][rows:, :], 3)
        bias.append(vectors[:1])
        wide[:1, at] = vectors[1:2]
        wide[1:2, at] = vectors[2:3]
    halo = list_ref.shape[1]
    start = 0
    for r in r_refs:
        depth = r.shape[0]
        sums[start : start + depth, :] = r[:, :full]
        for at in range(0, depth, RT):
            ids = r[at : at + RT, full:].astype(F32)[:, :1].astype(jnp.int32)
            names = list_ref[pl.ds(from_ref[(start + at) // RT], 1), :]
            found = ids == lax.broadcasted_iota(jnp.int32, (RT, halo), 1)
            node = jnp.sum(jnp.where(found, names.astype(F32), 0.0), axis=1, keepdims=True)
            node = jnp.where(ids >= 0, node, -1.0)
            nodes_of[start + at : start + at + RT, :] = jnp.broadcast_to(node, (RT, LANES))
        start += depth
    total = None
    for at in range(0, start, LANES):
        row = jnp.transpose(nodes_of[at : at + LANES, :])[:1].astype(jnp.int32)
        hot = row == lax.broadcasted_iota(jnp.int32, (rows, LANES), 0) + first
        hot = jnp.where(hot, 1.0, 0.0).astype(BF)
        part = jnp.dot(hot, sums[at : at + LANES, :], preferred_element_type=F32)
        total = part if total is None else total + part
    aggregated = total.astype(BF)
    nodes = n_all[...]
    mixed = [None] * pairs
    for k in range(pairs):
        for copy in copies[k]:
            copy.wait()
        pre = jnp.dot(nodes, store[k, :full, :], preferred_element_type=F32)
        pre += jnp.dot(aggregated, store[k, full : 2 * full, :], preferred_element_type=F32)
        hidden = silu(pre + bias[k]).astype(BF)
        for c in range(pairs):
            base = 2 * full + c * local
            part = jnp.dot(hidden, store[k, base : base + local, :], preferred_element_type=F32)
            mixed[c] = part if k == 0 else mixed[c] + part
    live = lax.broadcasted_iota(jnp.int32, (rows, 1), 0) + first < count_ref[0]
    mixed = jnp.concatenate(mixed, axis=1)
    n_all[...] = finish(mixed, nodes.astype(F32), wide[:1, :], wide[1:2, :], live)
    for k in range(pairs):
        at = pl.ds(pl.multiple_of((me ^ k) * local, local), local)
        outs[k][...] = n_all[:, at]


def layer(
    node_latents,
    edge_latents,
    edge_sender,
    edge_receiver,
    block_owner,
    node_counts,
    halo_nodes,
    w_endpoints,
    w_edge_in,
    edge_bias,
    w_edge_out,
    edge_gain,
    edge_shift,
    w_node_in,
    node_bias,
    w_node_out,
    node_gain,
    node_shift,
):
    patches = lax.axis_size("patch")
    pairs = lax.axis_size("pair")
    patch = lax.axis_index("patch").astype(jnp.int32)
    me = lax.axis_index("pair").astype(jnp.int32)
    full, local = w_edge_in.shape
    node_total = node_latents.shape[0]
    edge_total = edge_latents.shape[0]
    blocks, tile = edge_sender.shape
    halo = halo_nodes.shape[2]
    mine = blocks // pairs
    rows = edge_total // pairs
    quarter = node_total // pairs
    if pairs != 4 or patches % 2 or mine % 2:
        raise ValueError("unsupported mesh")
    peers = jnp.arange(pairs, dtype=jnp.int32) ^ me
    odd = patch % 2
    by_swap = patches <= 8 and halo % LANES == 0
    direct = blocks == patches and mine == 2
    order = jnp.arange(patches, dtype=jnp.int32)
    order = order ^ patch if by_swap else order

    def to_pairs(pieces):
        far = {k: swap(pieces[k], "pair", k) for k in (2, 3, 1)}
        return [pieces[0]] + [far[k] for k in range(1, pairs)]

    send_list = halo_nodes[0]
    if by_swap:
        picked = pick_rows(order, send_list, [node_latents], halo)
        table = [picked[0]] + [swap(picked[k], "patch", k) for k in range(1, patches)]
    else:
        groups = patches * halo // 256
        flat = send_list.reshape(groups, 256)
        picked = pick_rows(jnp.arange(groups, dtype=jnp.int32), flat, [node_latents], 256)
        table = [lax.all_to_all(jnp.concatenate(picked, axis=0), "patch", 0, 0, tiled=True)]

    def gather_slices(packed, *pieces):
        parts = [packed, swap(packed, "pair", 1)]
        far, far_core = [], []
        for piece in pieces:
            near = swap(piece, "pair", 2)
            other = swap(near, "patch", 1)
            far += [near, other]
            far_core += [swap(near, "pair", 1), swap(other, "pair", 1)]
        return parts + far + far_core

    flags = jnp.stack([me, odd, odd if direct else 0 * odd])
    e_chunks = ((0, 2 * full), (2 * full, 2 * full))
    ends = w_endpoints.reshape(2 * full, local)
    e_weights = gather_slices(*pack(pack_edge_kernel, odd.reshape(1), e_chunks, w_edge_in, ends, w_edge_out))
    e_vectors = jnp.stack([edge_bias, edge_gain, edge_shift])
    n_vectors = jnp.stack([node_bias, node_gain, node_shift])

    if direct:
        spots = jnp.arange(blocks, dtype=jnp.int32)
        block_at = jnp.sum(jnp.where(block_owner[None, :] == spots[:, None], spots[None, :], 0), axis=1)
    else:
        block_at = jnp.arange(blocks, dtype=jnp.int32)
    pair_blocks = block_at.reshape(pairs, mine)[peers].reshape(-1)

    previous = jnp.concatenate([jnp.full((blocks, 1), -2, jnp.int32), edge_receiver[:, :-1]], axis=1)
    segment = jnp.cumsum((edge_receiver != previous).astype(jnp.int32), axis=1) - 1
    segment = jnp.where(edge_receiver >= 0, segment, RT)
    member = segment[:, None, :] == jnp.arange(RT, dtype=jnp.int32)[None, :, None]
    tile_ids = jnp.max(jnp.where(member, edge_receiver[:, None, :], -1), axis=2)

    def place(owner):
        return (owner ^ patch if by_swap else owner) * halo

    sender = jnp.maximum(edge_sender, 0)
    sender_at = place(sender // halo) + sender % halo
    receiver_at = place(block_owner)[:, None] + jnp.maximum(tile_ids, 0)
    short = -(mine * RT) % LANES
    wanted = jnp.concatenate(
        [
            sender_at[pair_blocks].reshape(pairs, rows),
            receiver_at[pair_blocks].reshape(pairs, mine * RT),
            jnp.zeros((pairs, short), jnp.int32),
        ],
        axis=1,
    )
    my_blocks = pair_blocks[:mine]
    my_segment = segment[my_blocks]
    my_ids = jnp.broadcast_to(tile_ids[my_blocks].reshape(-1, 1), (mine * RT, LANES)).astype(BF)

    e_parts = to_pairs(split(pair_blocks, tile, mine, edge_latents, e_vectors))
    groups = jnp.arange(pairs, dtype=jnp.int32)
    seen = pick_rows(groups, wanted, table, rows + mine * RT)
    s_parts = to_pairs(seen)

    wide = full + LANES
    results = pl.pallas_call(
        functools.partial(edge_kernel, pairs, mine, e_chunks),
        in_specs=[SMEM] + [VMEM] * (2 + 2 * pairs) + [ANY] * len(e_weights),
        out_specs=[VMEM] * (pairs + mine),
        out_shape=[jax.ShapeDtypeStruct((rows, local), BF)] * pairs
        + [jax.ShapeDtypeStruct((RT, wide), BF)] * mine,
        scratch_shapes=[
            pltpu.VMEM((rows, 2 * full), BF),
            pltpu.VMEM((mine * RT, full), BF),
            pltpu.VMEM((rows, full), BF),
            pltpu.VMEM((rows, full), BF),
            pltpu.VMEM((8, full), F32),
            pltpu.VMEM((pairs, 4 * full, local), BF),
            pltpu.SemaphoreType.DMA((len(e_weights),)),
        ],
        cost_estimate=pl.CostEstimate(
            flops=6 * rows * full * full, bytes_accessed=10 * full * full, transcendentals=rows * full
        ),
    )(
        flags,
        my_segment,
        my_ids,
        *e_parts,
        *s_parts,
        *e_weights,
    )
    new_edges, sums = results[:pairs], results[pairs:]

    if direct:
        got = []
        for t in range(mine):
            route = []
            for p in range(patches):
                for j in range(pairs):
                    to = (j * mine + (p % 2 ^ t)) * pairs + p // mine
                    route.append((p * pairs + j, to))
            got.append(lax.ppermute(sums[t], ("patch", "pair"), route))
        got = to_pairs([jnp.concatenate(got, axis=0)] * pairs)
        near = jnp.stack([odd, 1 - odd])
        sources = (peers[:, None] * mine + near[None, :]).reshape(-1)
    else:
        all_sums = jnp.stack(to_pairs([jnp.stack(sums)] * pairs)).reshape(blocks, RT * wide)
        owners = block_owner.reshape(pairs, mine)[peers].reshape(-1)
        take = owners[None, :] == jnp.arange(patches, dtype=jnp.int32)[:, None]
        sent = jnp.dot(take.astype(BF), all_sums, preferred_element_type=F32).reshape(patches, RT, wide)
        none = jnp.any(take, axis=1)[:, None, None] | (jnp.arange(wide)[None, None, :] < full)
        sent = jnp.where(none, sent, -1.0).astype(BF)
        got = [lax.all_to_all(sent, "patch", 0, 0, tiled=True).reshape(patches * RT, wide)]
        sources = jnp.arange(patches, dtype=jnp.int32)

    new_edges = to_pairs(new_edges)
    edges_out = join(pair_blocks, tile, mine, new_edges)

    n_chunks = ((0, 2 * full), (2 * full, full))
    n_weights = gather_slices(
        *pack(pack_node_kernel, odd.reshape(1), n_chunks, w_node_in.reshape(2 * full, local), w_node_out)
    )
    n_parts = to_pairs(split(peers, quarter, 1, node_latents, n_vectors))
    new_nodes = pl.pallas_call(
        functools.partial(node_kernel, pairs, len(got), n_chunks),
        in_specs=[SMEM] * 3 + [VMEM] * (1 + pairs + len(got)) + [ANY] * len(n_weights),
        out_specs=[VMEM] * pairs,
        out_shape=[jax.ShapeDtypeStruct((quarter, local), BF)] * pairs,
        scratch_shapes=[
            pltpu.VMEM((quarter, full), BF),
            pltpu.VMEM((patches * RT, full), BF),
            pltpu.VMEM((patches * RT, LANES), F32),
            pltpu.VMEM((8, full), F32),
            pltpu.VMEM((pairs, 3 * full, local), BF),
            pltpu.SemaphoreType.DMA((len(n_weights),)),
        ],
        cost_estimate=pl.CostEstimate(
            flops=6 * quarter * full * full, bytes_accessed=8 * full * full, transcendentals=quarter * full
        ),
    )(
        flags,
        node_counts,
        sources,
        send_list,
        *n_parts,
        *got,
        *n_weights,
    )
    nodes_out = join(peers, quarter, 1, to_pairs(new_nodes))
    return (nodes_out, edges_out)


def solution(mesh):
    return jax.shard_map(
        layer,
        mesh=mesh,
        in_specs=(
            P("patch", "pair"),
            P("patch", "pair"),
            P("patch", None),
            P("patch", None),
            P("patch"),
            P("patch"),
            P("patch", None, None),
            P(None, None, "pair"),
            P(None, "pair"),
            P("pair"),
            P("pair", None),
            P("pair"),
            P("pair"),
            P(None, None, "pair"),
            P("pair"),
            P("pair", None),
            P("pair"),
            P("pair"),
        ),
        out_specs=(P("patch", "pair"), P("patch", "pair")),
        check_vma=False,
    )
```

```python
import functools

import jax
import jax.numpy as jnp
from jax import lax
from jax.experimental import pallas as pl
from jax.experimental.pallas import tpu as pltpu
from jax.sharding import PartitionSpec as P

RT = 16
EPS = 1e-05
LANES = 128
TAIL = 16
QUARTERS = 4


BF = jnp.bfloat16
F32 = jnp.float32
VMEM = pl.BlockSpec(memory_space=pltpu.VMEM)
SMEM = pl.BlockSpec(memory_space=pltpu.SMEM)
ANY = pl.BlockSpec(memory_space=pl.ANY)


def swap(value, axis, mask):
    size = lax.axis_size(axis)
    return lax.ppermute(value, axis, [(i, i ^ mask) for i in range(size)])


def grant(mib):
    return pltpu.CompilerParams(vmem_limit_bytes=mib * 2**20)


def column(row):
    wide = jnp.broadcast_to(row.astype(F32), (LANES, row.shape[1]))
    return jnp.transpose(wide).astype(jnp.int32)


def hot_lanes(index, start, count):
    parts = []
    for at in range(0, count, LANES):
        width = min(LANES, count - at)
        lane = lax.broadcasted_iota(jnp.int32, (index.shape[0], width), 1) + (start + at)
        parts.append(jnp.where(index[:, :width] == lane, 1.0, 0.0).astype(BF))
    return parts[0] if len(parts) == 1 else jnp.concatenate(parts, axis=1)


def gather_rows(index, tables):
    total = None
    start = 0
    for table in tables:
        hot = hot_lanes(index, start, table.shape[0])
        part = jnp.dot(hot, table[...], preferred_element_type=F32)
        total = part if total is None else total + part
        start += table.shape[0]
    return total.astype(BF)


def halo_kernel(by_swap, index_ref, table_ref, *outs):
    patch = lax.axis_index("patch")
    for g, out in enumerate(outs):
        row = index_ref[pl.ds(patch ^ g if by_swap else g, 1), :]
        out[...] = gather_rows(column(row), [table_ref])


def halo_rows(by_swap, index, table):
    groups, rows = index.shape
    depth, width = table.shape
    return pl.pallas_call(
        functools.partial(halo_kernel, by_swap),
        in_specs=[VMEM] * 2,
        out_specs=[VMEM] * groups,
        out_shape=[jax.ShapeDtypeStruct((rows, width), BF)] * groups,
        cost_estimate=pl.CostEstimate(
            flops=2 * groups * rows * depth * width, bytes_accessed=4 * rows * width, transcendentals=0
        ),
    )(index, table)


def block_of(owner_ref, spot, direct):
    if not direct:
        return spot
    found = 0
    for b in range(owner_ref.shape[0]):
        found = found + jnp.where(owner_ref[b] == spot, b, 0)
    return found


def sender_kernel(by_swap, direct, pairs, halo, owner_ref, sender_ref, receiver_ref, *refs):
    tables, refs = refs[:-(pairs + 2)], refs[-(pairs + 2) :]
    outs, segment_ref, ids_ref, changes = refs[:pairs], refs[pairs], refs[pairs + 1], None
    patch = lax.axis_index("patch")
    me = lax.axis_index("pair")
    blocks, tile = sender_ref.shape
    mine = blocks // pairs
    receiver = receiver_ref[...]
    lane = lax.broadcasted_iota(jnp.int32, (blocks, tile), 1)
    changes = (receiver != pltpu.roll(receiver, 1, axis=1)) | (lane == 0)
    upper = lax.broadcasted_iota(jnp.int32, (tile, tile), 0) <= lax.broadcasted_iota(jnp.int32, (tile, tile), 1)
    count = jnp.dot(
        jnp.where(changes, 1.0, 0.0).astype(BF), jnp.where(upper, 1.0, 0.0).astype(BF), preferred_element_type=F32
    )
    segments = jnp.where(receiver >= 0, count.astype(jnp.int32) - 1, RT)
    segment_ref[...] = segments
    for k in range(pairs):
        index = []
        extra = []
        for i in range(mine):
            block = block_of(owner_ref, (me ^ k) * mine + i, direct)
            slot = jnp.maximum(sender_ref[pl.ds(block, 1), :], 0)
            index.append(column(slot ^ (patch * halo) if by_swap else slot))
            segment = segment_ref[pl.ds(block, 1), :]
            names = receiver_ref[pl.ds(block, 1), :].astype(F32)
            member = segment == lax.broadcasted_iota(jnp.int32, (RT, tile), 0)
            ids = jnp.max(jnp.where(member, names, -1.0), axis=1, keepdims=True)
            if k == 0:
                ids_ref[i * RT : (i + 1) * RT, :] = jnp.broadcast_to(ids, (RT, LANES)).astype(BF)
            owner = owner_ref[block]
            base = (owner ^ patch if by_swap else owner) * halo
            at = jnp.maximum(ids, 0.0).astype(jnp.int32) + base
            extra.append(jnp.broadcast_to(at, (RT, LANES)))
        outs[k][...] = gather_rows(jnp.concatenate(index + extra, axis=0), tables)


def sender_rows(by_swap, direct, pairs, halo, owner, sender, receiver, tables):
    blocks, tile = sender.shape
    width = tables[0].shape[1]
    mine = blocks // pairs
    rows = mine * (tile + RT)
    results = pl.pallas_call(
        functools.partial(sender_kernel, by_swap, direct, pairs, halo),
        compiler_params=grant(16),
        in_specs=[SMEM] + [VMEM] * (2 + len(tables)),
        out_specs=[VMEM] * (pairs + 2),
        out_shape=[jax.ShapeDtypeStruct((rows, width), BF)] * pairs
        + [
            jax.ShapeDtypeStruct((blocks, tile), jnp.int32),
            jax.ShapeDtypeStruct((mine * RT, LANES), BF),
        ],
        cost_estimate=pl.CostEstimate(
            flops=2 * pairs * rows * 2048 * width, bytes_accessed=4 * pairs * rows * width, transcendentals=0
        ),
    )(owner, sender, receiver, *tables)
    return results[:pairs], results[pairs], results[pairs + 1]


def split_kernel(size, per, direct, owner_ref, in_ref, bias_ref, gain_ref, shift_ref, *outs):
    value = jnp.concatenate([bias_ref[...], gain_ref[...], shift_ref[...]], axis=0)
    high = value.astype(BF).astype(F32)
    middle = (value - high).astype(BF).astype(F32)
    low = value - high - middle
    parts = [high, middle, low]
    parts.append(jnp.zeros((TAIL - 3 * value.shape[0], value.shape[1]), F32))
    tail = jnp.concatenate(parts, axis=0).astype(BF)
    me = lax.axis_index("pair")
    for k, out in enumerate(outs):
        for i in range(per):
            at = pl.multiple_of(block_of(owner_ref, (me ^ k) * per + i, direct) * size, size)
            out[i * size : (i + 1) * size, :] = in_ref[pl.ds(at, size), :]
        out[per * size :, :] = tail


def unpack_vectors(tail, count):
    wide = tail.astype(F32)
    return wide[:count] + wide[count : 2 * count] + wide[2 * count : 3 * count]


def split(owner, size, per, direct, parts, value, *vectors):
    return pl.pallas_call(
        functools.partial(split_kernel, size, per, direct),
        compiler_params=grant(12),
        in_specs=[SMEM] + [VMEM] * 4,
        out_specs=[VMEM] * parts,
        out_shape=[jax.ShapeDtypeStruct((size * per + TAIL, value.shape[1]), BF)] * parts,
    )(owner, value, *[v.reshape(1, -1) for v in vectors])


def join_kernel(size, per, direct, owner_ref, *refs):
    out = refs[-1]
    me = lax.axis_index("pair")
    for k, part in enumerate(refs[:-1]):
        for i in range(per):
            at = pl.multiple_of(block_of(owner_ref, (me ^ k) * per + i, direct) * size, size)
            out[pl.ds(at, size), :] = part[i * size : (i + 1) * size, :]


def join(owner, size, per, direct, values):
    return pl.pallas_call(
        functools.partial(join_kernel, size, per, direct),
        compiler_params=grant(12),
        in_specs=[SMEM] + [VMEM] * len(values),
        out_specs=VMEM,
        out_shape=jax.ShapeDtypeStruct((size * per * len(values), values[0].shape[1]), BF),
    )(owner, *values)


def part_rows(source, rows, put):
    step = 2 * LANES
    for side in range(2):
        lane = lax.broadcasted_iota(jnp.int32, (LANES, step), 1)
        row = lax.broadcasted_iota(jnp.int32, (LANES, step), 0)
        hot = jnp.where(lane == 2 * row + side, 1.0, 0.0).astype(BF)
        for n in range(rows // step):
            part = jnp.dot(hot, source[n * step : (n + 1) * step, :], preferred_element_type=F32)
            put(side, n * LANES, part.astype(BF))


def parted_kernel(ends_ref, out_ref):
    half = ends_ref.shape[0] // 2

    def put(side, at, value):
        out_ref[side * half + at : side * half + at + LANES, :] = value

    part_rows(ends_ref, ends_ref.shape[0], put)


def pieces_kernel(unit, in_ref, ends_ref, out_ref, node_ref, last_ref, e_piece, n_piece, ends, sems):
    a = lax.axis_index("patch") % QUARTERS
    full = node_ref.shape[0] // 2
    at = pl.multiple_of(a * unit, unit)
    below = pl.multiple_of(full + a * unit, unit)
    copies = [
        (ends_ref.at[pl.ds(pl.multiple_of(a * 2 * unit, 2 * unit), 2 * unit)], ends),
        (in_ref.at[pl.ds(at, unit)], e_piece.at[pl.ds(0, unit)]),
        (out_ref.at[:, pl.ds(at, unit)], e_piece.at[pl.ds(3 * unit, unit)]),
        (node_ref.at[pl.ds(at, unit)], n_piece.at[pl.ds(0, unit)]),
        (node_ref.at[pl.ds(below, unit)], n_piece.at[pl.ds(unit, unit)]),
        (last_ref.at[:, pl.ds(at, unit)], n_piece.at[pl.ds(2 * unit, unit)]),
    ]
    copies = [pltpu.make_async_copy(src, dst, sems.at[n]) for n, (src, dst) in enumerate(copies)]
    for copy in copies:
        copy.start()
    copies[0].wait()

    def put(side, row, value):
        base = (1 + side) * unit + row
        e_piece[base : base + LANES, :] = value

    part_rows(ends, 2 * unit, put)
    for copy in copies[1:]:
        copy.wait()


def silu(value):
    return value / (1.0 + jnp.exp(-value))


def finish(mixed, old, gain, shift, live):
    width = mixed.shape[1]
    mean = jnp.sum(mixed, axis=1, keepdims=True) / width
    square = jnp.sum(mixed * mixed, axis=1, keepdims=True) / width
    norm = (mixed - mean) * lax.rsqrt(square - mean * mean + EPS) * gain + shift
    return jnp.where(live, old + norm, old).astype(BF)


def far_spot(r, unit):
    quarter = (lax.axis_index("patch") % QUARTERS) ^ r
    return pl.ds(pl.multiple_of(quarter * unit, unit), unit)


def edge_kernel(pairs, groups, direct, owner_ref, segrow_ref, ids_ref, *refs):
    e_refs, refs = refs[:pairs], refs[pairs:]
    s_refs, refs = refs[:pairs], refs[pairs:]
    whole, far, refs = (refs[:3], refs[3:6]), (refs[6:10], refs[10:14]), refs[14:]
    outs, refs = refs[:pairs], refs[pairs:]
    sum_refs, refs = refs[:groups], refs[groups:]
    e_all, s_all, r_all, hidden, mixed_all, new_all, wide = refs
    me = lax.axis_index("pair")
    turn = lax.axis_index("patch") % 2 if direct else 0
    rows, full = new_all.shape
    local = full // pairs
    tile = rows // groups
    bias = []
    for k in range(pairs):
        at = pl.multiple_of((me ^ k) * local, local)
        s_all[:, pl.ds(at, local)] = s_refs[k][:rows, :]
        e_all[:, pl.ds(at, local)] = e_refs[k][:rows, :]
        r_all[:, pl.ds(at, local)] = s_refs[k][rows:, :]
        vectors = unpack_vectors(e_refs[k][rows:, :], 3)
        bias.append(vectors[:1])
        wide[:1, pl.ds(at, local)] = vectors[1:2]
        wide[1:2, pl.ds(at, local)] = vectors[2:3]
    segments, hots = [], []
    for g in range(groups):
        block = block_of(owner_ref, me * groups + g, direct)
        segment = column(segrow_ref[pl.ds(block, 1), :])
        segments.append(segment)
        hots.append(hot_lanes(segment, 0, RT))
    for k in range(pairs):
        if k < 2:
            w_edge, w_ends, _ = whole[k]
            receivers = jnp.dot(r_all[...], w_ends[full:, :], preferred_element_type=F32)
        else:
            receivers = None
            for r, piece in enumerate(far[k - 2]):
                part = r_all[:, far_spot(r, local)]
                part = jnp.dot(part, piece[2 * local : 3 * local, :], preferred_element_type=F32)
                receivers = part if receivers is None else receivers + part
        receivers = receivers.astype(BF)
        for g in range(groups):
            at = slice(g * tile, (g + 1) * tile)
            pre = jnp.dot(hots[g], receivers[g * RT : (g + 1) * RT], preferred_element_type=F32)
            if k < 2:
                pre += jnp.dot(e_all[at, :], w_edge[...], preferred_element_type=F32)
                pre += jnp.dot(s_all[at, :], w_ends[:full, :], preferred_element_type=F32)
            else:
                for r, piece in enumerate(far[k - 2]):
                    spot = far_spot(r, local)
                    pre += jnp.dot(e_all[at, spot], piece[:local, :], preferred_element_type=F32)
                    pre += jnp.dot(s_all[at, spot], piece[local : 2 * local, :], preferred_element_type=F32)
            hidden[at, k * local : (k + 1) * local] = silu(pre + bias[k]).astype(BF)
    for g in range(groups):
        at = slice(g * tile, (g + 1) * tile)
        first = hidden[at, :local], hidden[at, local : 2 * local]
        last = hidden[at, 2 * local : 3 * local], hidden[at, 3 * local :]
        for r in range(QUARTERS):
            spot = far_spot(r, local)
            total = None
            for near, (_, _, w_out), behind, pieces in zip(first, whole, last, far):
                part = jnp.dot(near, w_out[:, spot], preferred_element_type=F32)
                part += jnp.dot(behind, pieces[r][3 * local :, :], preferred_element_type=F32)
                total = part if total is None else total + part
            mixed_all[at, spot] = total
        live = segments[g][:, :1] < RT
        old = e_all[at, :].astype(F32)
        new_all[at, :] = finish(mixed_all[at, :], old, wide[:1, :], wide[1:2, :], live)
    for t in range(groups):
        g = t ^ turn
        segrow = segrow_ref[pl.ds(block_of(owner_ref, me * groups + g, direct), 1), :]
        member = segrow == lax.broadcasted_iota(jnp.int32, (RT, tile), 0)
        member = jnp.where(member, 1.0, 0.0).astype(BF)
        new = new_all[pl.ds(pl.multiple_of(g * tile, tile), tile), :]
        total = jnp.dot(member, new, preferred_element_type=F32)
        sum_refs[t][:, :full] = total.astype(BF)
        sum_refs[t][:, full:] = ids_ref[pl.ds(pl.multiple_of(g * RT, RT), RT), :]
    for k in range(pairs):
        at = pl.ds(pl.multiple_of((me ^ k) * local, local), local)
        outs[k][...] = new_all[:, at]


def node_kernel(pairs, sources, direct, count_ref, list_ref, *refs):
    n_refs, refs = refs[:pairs], refs[pairs:]
    r_refs, refs = refs[:sources], refs[sources:]
    whole, far, refs = (refs[:2], refs[2:4]), (refs[4:8], refs[8:12]), refs[12:]
    outs, refs = refs[:pairs], refs[pairs:]
    n_all, sums, nodes_of, aggregated, hidden, mixed_all, wide = refs
    me = lax.axis_index("pair")
    odd = lax.axis_index("patch") % 2
    rows, full = n_all.shape
    local = full // pairs
    first = me * rows
    bias = []
    for k in range(pairs):
        at = pl.ds(pl.multiple_of((me ^ k) * local, local), local)
        n_all[:, at] = n_refs[k][:rows, :]
        vectors = unpack_vectors(n_refs[k][rows:, :], 3)
        bias.append(vectors[:1])
        wide[:1, at] = vectors[1:2]
        wide[1:2, at] = vectors[2:3]
    halo = list_ref.shape[1]
    start = 0
    for r in r_refs:
        depth = r.shape[0]
        sums[start : start + depth, :] = r[:, :full]
        for at in range(0, depth, RT):
            ids = r[at : at + RT, full:].astype(F32)[:, :1].astype(jnp.int32)
            turn = (start + at) // RT
            if direct:
                turn = (me ^ (turn // 2)) * 2 + (odd ^ (turn % 2))
            names = list_ref[pl.ds(turn, 1), :]
            found = ids == lax.broadcasted_iota(jnp.int32, (RT, halo), 1)
            node = jnp.sum(jnp.where(found, names.astype(F32), 0.0), axis=1, keepdims=True)
            node = jnp.where(ids >= 0, node, -1.0)
            nodes_of[start + at : start + at + RT, :] = jnp.broadcast_to(node, (RT, LANES))
        start += depth
    total = None
    for at in range(0, start, LANES):
        row = jnp.transpose(nodes_of[at : at + LANES, :])[:1].astype(jnp.int32)
        hot = row == lax.broadcasted_iota(jnp.int32, (rows, LANES), 0) + first
        hot = jnp.where(hot, 1.0, 0.0).astype(BF)
        part = jnp.dot(hot, sums[at : at + LANES, :], preferred_element_type=F32)
        total = part if total is None else total + part
    aggregated[...] = total.astype(BF)
    for k in range(pairs):
        if k < 2:
            w_in = whole[k][0]
            pre = jnp.dot(n_all[...], w_in[:full, :], preferred_element_type=F32)
            pre += jnp.dot(aggregated[...], w_in[full:, :], preferred_element_type=F32)
        else:
            pre = None
            for r, piece in enumerate(far[k - 2]):
                spot = far_spot(r, local)
                part = jnp.dot(n_all[:, spot], piece[:local, :], preferred_element_type=F32)
                part += jnp.dot(aggregated[:, spot], piece[local : 2 * local, :], preferred_element_type=F32)
                pre = part if pre is None else pre + part
        hidden[:, k * local : (k + 1) * local] = silu(pre + bias[k]).astype(BF)
    for r in range(QUARTERS):
        spot = far_spot(r, local)
        total = None
        for k in range(2):
            part = jnp.dot(hidden[:, k * local : (k + 1) * local], whole[k][1][:, spot], preferred_element_type=F32)
            behind = hidden[:, (k + 2) * local : (k + 3) * local]
            part += jnp.dot(behind, far[k][r][2 * local :, :], preferred_element_type=F32)
            total = part if total is None else total + part
        mixed_all[:, spot] = total
    live = lax.broadcasted_iota(jnp.int32, (rows, 1), 0) + first < count_ref[0]
    n_all[...] = finish(mixed_all[...], n_all[...].astype(F32), wide[:1, :], wide[1:2, :], live)
    for k in range(pairs):
        at = pl.ds(pl.multiple_of((me ^ k) * local, local), local)
        outs[k][...] = n_all[:, at]


def layer(
    node_latents,
    edge_latents,
    edge_sender,
    edge_receiver,
    block_owner,
    node_counts,
    halo_nodes,
    w_endpoints,
    w_edge_in,
    edge_bias,
    w_edge_out,
    edge_gain,
    edge_shift,
    w_node_in,
    node_bias,
    w_node_out,
    node_gain,
    node_shift,
):
    patches = lax.axis_size("patch")
    pairs = lax.axis_size("pair")
    me = lax.axis_index("pair")
    full, local = w_edge_in.shape
    node_total = node_latents.shape[0]
    edge_total = edge_latents.shape[0]
    blocks, tile = edge_sender.shape
    halo = halo_nodes.shape[2]
    mine = blocks // pairs
    rows = edge_total // pairs
    quarter = node_total // pairs
    if pairs != QUARTERS or patches % QUARTERS or mine % 2 or halo & (halo - 1):
        raise ValueError("unsupported mesh")
    by_swap = patches <= 8 and halo % LANES == 0
    direct = blocks == patches and mine == 2

    def to_pairs(pieces):
        far = {k: swap(pieces[k], "pair", k) for k in (2, 3, 1)}
        return [pieces[0]] + [far[k] for k in range(1, pairs)]

    send_list = halo_nodes[0]
    if by_swap:
        picked = halo_rows(True, send_list, node_latents)
        table = [picked[0]] + [swap(picked[k], "patch", k) for k in range(1, patches)]
    else:
        picked = halo_rows(False, send_list.reshape(-1, 2 * LANES), node_latents)
        table = [lax.all_to_all(jnp.concatenate(picked, axis=0), "patch", 0, 0, tiled=True)]

    ends = w_endpoints.reshape(2 * full, local)
    w_nodes = w_node_in.reshape(2 * full, local)
    e_piece, n_piece = pl.pallas_call(
        functools.partial(pieces_kernel, local),
        compiler_params=grant(12),
        in_specs=[ANY] * 5,
        out_specs=[VMEM] * 2,
        out_shape=[jax.ShapeDtypeStruct((4 * local, local), BF), jax.ShapeDtypeStruct((3 * local, local), BF)],
        scratch_shapes=[pltpu.VMEM((2 * local, local), BF), pltpu.SemaphoreType.DMA((6,))],
    )(w_edge_in, ends, w_edge_out, w_nodes, w_node_out)
    parted = pl.pallas_call(
        parted_kernel,
        compiler_params=grant(12),
        in_specs=[VMEM],
        out_specs=VMEM,
        out_shape=jax.ShapeDtypeStruct((2 * full, local), BF),
    )(ends)

    def gather_slices(own, piece):
        parts = list(own) + [swap(w, "pair", 1) for w in own]
        near = swap(piece, "pair", 2)
        side = swap(near, "patch", 1)
        far = [near, side, swap(near, "patch", 2), swap(side, "patch", 2)]
        return parts + far + [swap(w, "pair", 1) for w in far]

    e_weights = gather_slices((w_edge_in, parted, w_edge_out), e_piece)
    n_weights = gather_slices((w_nodes, w_node_out), n_piece)

    e_parts = to_pairs(split(block_owner, tile, mine, direct, pairs, edge_latents, edge_bias, edge_gain, edge_shift))
    seen, segment, my_ids = sender_rows(by_swap, direct, pairs, halo, block_owner, edge_sender, edge_receiver, table)
    s_parts = to_pairs(seen)

    wide = full + LANES
    results = pl.pallas_call(
        functools.partial(edge_kernel, pairs, mine, direct),
        compiler_params=grant(28),
        in_specs=[SMEM] + [VMEM] * (2 + 2 * pairs + len(e_weights)),
        out_specs=[VMEM] * (pairs + mine),
        out_shape=[jax.ShapeDtypeStruct((rows, local), BF)] * pairs
        + [jax.ShapeDtypeStruct((RT, wide), BF)] * mine,
        scratch_shapes=[
            pltpu.VMEM((rows, full), BF),
            pltpu.VMEM((rows, full), BF),
            pltpu.VMEM((mine * RT, full), BF),
            pltpu.VMEM((rows, full), BF),
            pltpu.VMEM((rows, full), F32),
            pltpu.VMEM((rows, full), BF),
            pltpu.VMEM((8, full), F32),
        ],
        cost_estimate=pl.CostEstimate(
            flops=6 * rows * full * full, bytes_accessed=10 * full * full, transcendentals=rows * full
        ),
    )(
        block_owner,
        segment,
        my_ids,
        *e_parts,
        *s_parts,
        *e_weights,
    )
    new_edges, sums = results[:pairs], results[pairs:]

    if direct:
        got = []
        for t in range(mine):
            route = []
            for p in range(patches):
                for j in range(pairs):
                    to = (j * mine + (p % 2 ^ t)) * pairs + p // mine
                    route.append((p * pairs + j, to))
            got.append(lax.ppermute(sums[t], ("patch", "pair"), route))
        got = to_pairs([jnp.concatenate(got, axis=0)] * pairs)
    else:
        all_sums = jnp.stack(to_pairs([jnp.stack(sums)] * pairs)).reshape(blocks, RT * wide)
        peers = jnp.arange(pairs, dtype=jnp.int32) ^ me
        owners = block_owner.reshape(pairs, mine)[peers].reshape(-1)
        take = owners[None, :] == jnp.arange(patches, dtype=jnp.int32)[:, None]
        sent = jnp.dot(take.astype(BF), all_sums, preferred_element_type=F32).reshape(patches, RT, wide)
        none = jnp.any(take, axis=1)[:, None, None] | (jnp.arange(wide)[None, None, :] < full)
        sent = jnp.where(none, sent, -1.0).astype(BF)
        got = [lax.all_to_all(sent, "patch", 0, 0, tiled=True).reshape(patches * RT, wide)]

    new_edges = to_pairs(new_edges)
    edges_out = join(block_owner, tile, mine, direct, new_edges)

    n_parts = to_pairs(split(node_counts, quarter, 1, False, pairs, node_latents, node_bias, node_gain, node_shift))
    new_nodes = pl.pallas_call(
        functools.partial(node_kernel, pairs, len(got), direct),
        compiler_params=grant(20),
        in_specs=[SMEM] + [VMEM] * (1 + pairs + len(got) + len(n_weights)),
        out_specs=[VMEM] * pairs,
        out_shape=[jax.ShapeDtypeStruct((quarter, local), BF)] * pairs,
        scratch_shapes=[
            pltpu.VMEM((quarter, full), BF),
            pltpu.VMEM((patches * RT, full), BF),
            pltpu.VMEM((patches * RT, LANES), F32),
            pltpu.VMEM((quarter, full), BF),
            pltpu.VMEM((quarter, full), BF),
            pltpu.VMEM((quarter, full), F32),
            pltpu.VMEM((8, full), F32),
        ],
        cost_estimate=pl.CostEstimate(
            flops=6 * quarter * full * full, bytes_accessed=8 * full * full, transcendentals=quarter * full
        ),
    )(
        node_counts,
        send_list,
        *n_parts,
        *got,
        *n_weights,
    )
    nodes_out = join(node_counts, quarter, 1, False, to_pairs(new_nodes))
    return (nodes_out, edges_out)


def solution(mesh):
    return jax.shard_map(
        layer,
        mesh=mesh,
        in_specs=(
            P("patch", "pair"),
            P("patch", "pair"),
            P("patch", None),
            P("patch", None),
            P("patch"),
            P("patch"),
            P("patch", None, None),
            P(None, None, "pair"),
            P(None, "pair"),
            P("pair"),
            P("pair", None),
            P("pair"),
            P("pair"),
            P(None, None, "pair"),
            P("pair"),
            P("pair", None),
            P("pair"),
            P("pair"),
        ),
        out_specs=(P("patch", "pair"), P("patch", "pair")),
        check_vma=False,
    )
```

```python
import functools

import jax
import jax.numpy as jnp
from jax import lax
from jax.experimental import pallas as pl
from jax.experimental.pallas import tpu as pltpu
from jax.sharding import PartitionSpec as P

RT = 16
EPS = 1e-05
LANES = 128
TAIL = 16
QUARTERS = 4


BF = jnp.bfloat16
F32 = jnp.float32
VMEM = pl.BlockSpec(memory_space=pltpu.VMEM)
SMEM = pl.BlockSpec(memory_space=pltpu.SMEM)
HBM = pl.BlockSpec(memory_space=pltpu.HBM)


def swap(value, axis, mask):
    size = lax.axis_size(axis)
    return lax.ppermute(value, axis, [(i, i ^ mask) for i in range(size)])


def grant(mib):
    return pltpu.CompilerParams(vmem_limit_bytes=mib * 2**20)


def column(row):
    wide = jnp.broadcast_to(row.astype(F32), (LANES, row.shape[1]))
    return jnp.transpose(wide).astype(jnp.int32)


def hot_lanes(index, start, count):
    parts = []
    for at in range(0, count, LANES):
        width = min(LANES, count - at)
        lane = lax.broadcasted_iota(jnp.int32, (index.shape[0], width), 1) + (start + at)
        parts.append(jnp.where(index[:, :width] == lane, 1.0, 0.0).astype(BF))
    return parts[0] if len(parts) == 1 else jnp.concatenate(parts, axis=1)


def gather_rows(index, tables):
    total = None
    start = 0
    for table in tables:
        hot = hot_lanes(index, start, table.shape[0])
        part = jnp.dot(hot, table[...], preferred_element_type=F32)
        total = part if total is None else total + part
        start += table.shape[0]
    return total.astype(BF)


def halo_kernel(by_swap, index_ref, table_ref, *outs):
    patch = lax.axis_index("patch")
    for g, out in enumerate(outs):
        row = index_ref[pl.ds(patch ^ g if by_swap else g, 1), :]
        out[...] = gather_rows(column(row), [table_ref])


def halo_rows(by_swap, index, table):
    groups, rows = index.shape
    depth, width = table.shape
    return pl.pallas_call(
        functools.partial(halo_kernel, by_swap),
        in_specs=[VMEM] * 2,
        out_specs=[VMEM] * groups,
        out_shape=[jax.ShapeDtypeStruct((rows, width), BF)] * groups,
        cost_estimate=pl.CostEstimate(
            flops=2 * groups * rows * depth * width, bytes_accessed=4 * rows * width, transcendentals=0
        ),
    )(index, table)


def block_of(owner_ref, spot, direct):
    if not direct:
        return spot
    found = 0
    for b in range(owner_ref.shape[0]):
        found = found + jnp.where(owner_ref[b] == spot, b, 0)
    return found


def sender_kernel(by_swap, direct, pairs, halo, owner_ref, sender_ref, receiver_ref, *refs):
    tables, refs = refs[:-(pairs + 2)], refs[-(pairs + 2) :]
    outs, segment_ref, ids_ref, changes = refs[:pairs], refs[pairs], refs[pairs + 1], None
    patch = lax.axis_index("patch")
    me = lax.axis_index("pair")
    blocks, tile = sender_ref.shape
    mine = blocks // pairs
    receiver = receiver_ref[...]
    lane = lax.broadcasted_iota(jnp.int32, (blocks, tile), 1)
    changes = (receiver != pltpu.roll(receiver, 1, axis=1)) | (lane == 0)
    upper = lax.broadcasted_iota(jnp.int32, (tile, tile), 0) <= lax.broadcasted_iota(jnp.int32, (tile, tile), 1)
    count = jnp.dot(
        jnp.where(changes, 1.0, 0.0).astype(BF), jnp.where(upper, 1.0, 0.0).astype(BF), preferred_element_type=F32
    )
    segments = jnp.where(receiver >= 0, count.astype(jnp.int32) - 1, RT)
    segment_ref[...] = segments
    for k in range(pairs):
        index = []
        extra = []
        for i in range(mine):
            block = block_of(owner_ref, (me ^ k) * mine + i, direct)
            slot = jnp.maximum(sender_ref[pl.ds(block, 1), :], 0)
            index.append(column(slot ^ (patch * halo) if by_swap else slot))
            segment = segment_ref[pl.ds(block, 1), :]
            names = receiver_ref[pl.ds(block, 1), :].astype(F32)
            member = segment == lax.broadcasted_iota(jnp.int32, (RT, tile), 0)
            ids = jnp.max(jnp.where(member, names, -1.0), axis=1, keepdims=True)
            if k == 0:
                ids_ref[i * RT : (i + 1) * RT, :] = jnp.broadcast_to(ids, (RT, LANES)).astype(BF)
            owner = owner_ref[block]
            base = (owner ^ patch if by_swap else owner) * halo
            at = jnp.maximum(ids, 0.0).astype(jnp.int32) + base
            extra.append(jnp.broadcast_to(at, (RT, LANES)))
        outs[k][...] = gather_rows(jnp.concatenate(index + extra, axis=0), tables)


def sender_rows(by_swap, direct, pairs, halo, owner, sender, receiver, tables):
    blocks, tile = sender.shape
    width = tables[0].shape[1]
    mine = blocks // pairs
    rows = mine * (tile + RT)
    results = pl.pallas_call(
        functools.partial(sender_kernel, by_swap, direct, pairs, halo),
        compiler_params=grant(16),
        in_specs=[SMEM] + [VMEM] * (2 + len(tables)),
        out_specs=[VMEM] * (pairs + 2),
        out_shape=[jax.ShapeDtypeStruct((rows, width), BF)] * pairs
        + [
            jax.ShapeDtypeStruct((blocks, tile), jnp.int32),
            jax.ShapeDtypeStruct((mine * RT, LANES), BF),
        ],
        cost_estimate=pl.CostEstimate(
            flops=2 * pairs * rows * 2048 * width, bytes_accessed=4 * pairs * rows * width, transcendentals=0
        ),
    )(owner, sender, receiver, *tables)
    return results[:pairs], results[pairs], results[pairs + 1]


def split_kernel(size, per, direct, owner_ref, in_ref, bias_ref, gain_ref, shift_ref, *outs):
    value = jnp.concatenate([bias_ref[...], gain_ref[...], shift_ref[...]], axis=0)
    high = value.astype(BF).astype(F32)
    middle = (value - high).astype(BF).astype(F32)
    low = value - high - middle
    parts = [high, middle, low]
    parts.append(jnp.zeros((TAIL - 3 * value.shape[0], value.shape[1]), F32))
    tail = jnp.concatenate(parts, axis=0).astype(BF)
    me = lax.axis_index("pair")
    for k, out in enumerate(outs):
        for i in range(per):
            at = pl.multiple_of(block_of(owner_ref, (me ^ k) * per + i, direct) * size, size)
            out[i * size : (i + 1) * size, :] = in_ref[pl.ds(at, size), :]
        out[per * size :, :] = tail


def unpack_vectors(tail, count):
    wide = tail.astype(F32)
    return wide[:count] + wide[count : 2 * count] + wide[2 * count : 3 * count]


def split(owner, size, per, direct, parts, value, *vectors):
    return pl.pallas_call(
        functools.partial(split_kernel, size, per, direct),
        compiler_params=grant(12),
        in_specs=[SMEM] + [VMEM] * 4,
        out_specs=[VMEM] * parts,
        out_shape=[jax.ShapeDtypeStruct((size * per + TAIL, value.shape[1]), BF)] * parts,
    )(owner, value, *[v.reshape(1, -1) for v in vectors])


def join_kernel(size, per, direct, owner_ref, *refs):
    out = refs[-1]
    me = lax.axis_index("pair")
    for k, part in enumerate(refs[:-1]):
        for i in range(per):
            at = pl.multiple_of(block_of(owner_ref, (me ^ k) * per + i, direct) * size, size)
            out[pl.ds(at, size), :] = part[i * size : (i + 1) * size, :]


def join(owner, size, per, direct, values):
    return pl.pallas_call(
        functools.partial(join_kernel, size, per, direct),
        compiler_params=grant(12),
        in_specs=[SMEM] + [VMEM] * len(values),
        out_specs=VMEM,
        out_shape=jax.ShapeDtypeStruct((size * per * len(values), values[0].shape[1]), BF),
    )(owner, *values)


def parted_kernel(ends_ref, out_ref):
    full = ends_ref.shape[0]
    for side in range(2):
        out_ref[side * full : (side + 1) * full, :] = ends_ref[:, side, :]


def pieces_kernel(unit, in_ref, ends_ref, out_ref, node_ref, last_ref, e_piece, n_piece, ends, sems):
    a = lax.axis_index("patch") % QUARTERS
    full = node_ref.shape[0] // 2
    at = pl.multiple_of(a * unit, unit)
    below = pl.multiple_of(full + a * unit, unit)
    copies = [
        (ends_ref.at[pl.ds(at, unit)], ends),
        (in_ref.at[pl.ds(at, unit)], e_piece.at[pl.ds(0, unit)]),
        (out_ref.at[:, pl.ds(at, unit)], e_piece.at[pl.ds(3 * unit, unit)]),
        (node_ref.at[pl.ds(at, unit)], n_piece.at[pl.ds(0, unit)]),
        (node_ref.at[pl.ds(below, unit)], n_piece.at[pl.ds(unit, unit)]),
        (last_ref.at[:, pl.ds(at, unit)], n_piece.at[pl.ds(2 * unit, unit)]),
    ]
    copies = [pltpu.make_async_copy(src, dst, sems.at[n]) for n, (src, dst) in enumerate(copies)]
    for copy in copies:
        copy.start()
    copies[0].wait()
    for side in range(2):
        e_piece[(1 + side) * unit : (2 + side) * unit, :] = ends[:, side, :]
    for copy in copies[1:]:
        copy.wait()


def silu(value):
    return value / (1.0 + jnp.exp(-value))


def finish(mixed, old, gain, shift, live):
    width = mixed.shape[1]
    mean = jnp.sum(mixed, axis=1, keepdims=True) / width
    square = jnp.sum(mixed * mixed, axis=1, keepdims=True) / width
    norm = (mixed - mean) * lax.rsqrt(square - mean * mean + EPS) * gain + shift
    return jnp.where(live, old + norm, old).astype(BF)


def far_spot(r, unit):
    quarter = (lax.axis_index("patch") % QUARTERS) ^ r
    return pl.ds(pl.multiple_of(quarter * unit, unit), unit)


def far_parts(pieces, unit):
    parts = [[piece.at[pl.ds(n * unit, unit)] for n in range(piece.shape[0] // unit)] for piece in pieces]
    return parts[:-2] + [parts[-2] + parts[-1]]


def edge_kernel(pairs, groups, direct, owner_ref, segrow_ref, ids_ref, *refs):
    e_refs, refs = refs[:pairs], refs[pairs:]
    s_refs, refs = refs[:pairs], refs[pairs:]
    whole, far, refs = (refs[:3], refs[3:6]), (refs[6:11], refs[11:16]), refs[16:]
    far = [far_parts(pieces, refs[0].shape[1]) for pieces in far]
    outs, refs = refs[:pairs], refs[pairs:]
    sum_refs, refs = refs[:groups], refs[groups:]
    e_all, s_all, r_all, hidden, mixed_all, new_all, wide = refs
    me = lax.axis_index("pair")
    turn = lax.axis_index("patch") % 2 if direct else 0
    rows, full = new_all.shape
    local = full // pairs
    tile = rows // groups
    bias = []
    for k in range(pairs):
        at = pl.multiple_of((me ^ k) * local, local)
        s_all[:, pl.ds(at, local)] = s_refs[k][:rows, :]
        e_all[:, pl.ds(at, local)] = e_refs[k][:rows, :]
        r_all[:, pl.ds(at, local)] = s_refs[k][rows:, :]
        vectors = unpack_vectors(e_refs[k][rows:, :], 3)
        bias.append(vectors[:1])
        wide[:1, pl.ds(at, local)] = vectors[1:2]
        wide[1:2, pl.ds(at, local)] = vectors[2:3]
    segments, hots = [], []
    for g in range(groups):
        block = block_of(owner_ref, me * groups + g, direct)
        segment = column(segrow_ref[pl.ds(block, 1), :])
        segments.append(segment)
        hots.append(hot_lanes(segment, 0, RT))
    for k in range(pairs):
        if k < 2:
            w_edge, w_ends, _ = whole[k]
            receivers = jnp.dot(r_all[...], w_ends[full:, :], preferred_element_type=F32)
        else:
            receivers = None
            for r, piece in enumerate(far[k - 2]):
                part = r_all[:, far_spot(r, local)]
                part = jnp.dot(part, piece[2][...], preferred_element_type=F32)
                receivers = part if receivers is None else receivers + part
        receivers = receivers.astype(BF)
        for g in range(groups):
            at = slice(g * tile, (g + 1) * tile)
            pre = jnp.dot(hots[g], receivers[g * RT : (g + 1) * RT], preferred_element_type=F32)
            if k < 2:
                pre += jnp.dot(e_all[at, :], w_edge[...], preferred_element_type=F32)
                pre += jnp.dot(s_all[at, :], w_ends[:full, :], preferred_element_type=F32)
            else:
                for r, piece in enumerate(far[k - 2]):
                    spot = far_spot(r, local)
                    pre += jnp.dot(e_all[at, spot], piece[0][...], preferred_element_type=F32)
                    pre += jnp.dot(s_all[at, spot], piece[1][...], preferred_element_type=F32)
            hidden[at, k * local : (k + 1) * local] = silu(pre + bias[k]).astype(BF)
    for g in range(groups):
        at = slice(g * tile, (g + 1) * tile)
        first = hidden[at, :local], hidden[at, local : 2 * local]
        last = hidden[at, 2 * local : 3 * local], hidden[at, 3 * local :]
        for r in range(QUARTERS):
            spot = far_spot(r, local)
            total = None
            for near, (_, _, w_out), behind, pieces in zip(first, whole, last, far):
                part = jnp.dot(near, w_out[:, spot], preferred_element_type=F32)
                part += jnp.dot(behind, pieces[r][3][...], preferred_element_type=F32)
                total = part if total is None else total + part
            mixed_all[at, spot] = total
        live = segments[g][:, :1] < RT
        old = e_all[at, :].astype(F32)
        new_all[at, :] = finish(mixed_all[at, :], old, wide[:1, :], wide[1:2, :], live)
    for t in range(groups):
        g = t ^ turn
        segrow = segrow_ref[pl.ds(block_of(owner_ref, me * groups + g, direct), 1), :]
        member = segrow == lax.broadcasted_iota(jnp.int32, (RT, tile), 0)
        member = jnp.where(member, 1.0, 0.0).astype(BF)
        new = new_all[pl.ds(pl.multiple_of(g * tile, tile), tile), :]
        total = jnp.dot(member, new, preferred_element_type=F32)
        sum_refs[t][:, :full] = total.astype(BF)
        sum_refs[t][:, full:] = ids_ref[pl.ds(pl.multiple_of(g * RT, RT), RT), :]
    for k in range(pairs):
        at = pl.ds(pl.multiple_of((me ^ k) * local, local), local)
        outs[k][...] = new_all[:, at]


def node_kernel(pairs, sources, direct, count_ref, list_ref, *refs):
    n_refs, refs = refs[:pairs], refs[pairs:]
    r_refs, refs = refs[:sources], refs[sources:]
    whole, far, refs = (refs[:2], refs[2:4]), (refs[4:8], refs[8:12]), refs[12:]
    outs, refs = refs[:pairs], refs[pairs:]
    n_all, sums, nodes_of, aggregated, hidden, mixed_all, wide = refs
    me = lax.axis_index("pair")
    odd = lax.axis_index("patch") % 2
    rows, full = n_all.shape
    local = full // pairs
    first = me * rows
    bias = []
    for k in range(pairs):
        at = pl.ds(pl.multiple_of((me ^ k) * local, local), local)
        n_all[:, at] = n_refs[k][:rows, :]
        vectors = unpack_vectors(n_refs[k][rows:, :], 3)
        bias.append(vectors[:1])
        wide[:1, at] = vectors[1:2]
        wide[1:2, at] = vectors[2:3]
    halo = list_ref.shape[1]
    start = 0
    for r in r_refs:
        depth = r.shape[0]
        sums[start : start + depth, :] = r[:, :full]
        for at in range(0, depth, RT):
            ids = r[at : at + RT, full:].astype(F32)[:, :1].astype(jnp.int32)
            turn = (start + at) // RT
            if direct:
                turn = (me ^ (turn // 2)) * 2 + (odd ^ (turn % 2))
            names = list_ref[pl.ds(turn, 1), :]
            found = ids == lax.broadcasted_iota(jnp.int32, (RT, halo), 1)
            node = jnp.sum(jnp.where(found, names.astype(F32), 0.0), axis=1, keepdims=True)
            node = jnp.where(ids >= 0, node, -1.0)
            nodes_of[start + at : start + at + RT, :] = jnp.broadcast_to(node, (RT, LANES))
        start += depth
    total = None
    for at in range(0, start, LANES):
        row = jnp.transpose(nodes_of[at : at + LANES, :])[:1].astype(jnp.int32)
        hot = row == lax.broadcasted_iota(jnp.int32, (rows, LANES), 0) + first
        hot = jnp.where(hot, 1.0, 0.0).astype(BF)
        part = jnp.dot(hot, sums[at : at + LANES, :], preferred_element_type=F32)
        total = part if total is None else total + part
    aggregated[...] = total.astype(BF)
    for k in range(pairs):
        if k < 2:
            w_in = whole[k][0]
            pre = jnp.dot(n_all[...], w_in[:full, :], preferred_element_type=F32)
            pre += jnp.dot(aggregated[...], w_in[full:, :], preferred_element_type=F32)
        else:
            pre = None
            for r, piece in enumerate(far[k - 2]):
                spot = far_spot(r, local)
                part = jnp.dot(n_all[:, spot], piece[:local, :], preferred_element_type=F32)
                part += jnp.dot(aggregated[:, spot], piece[local : 2 * local, :], preferred_element_type=F32)
                pre = part if pre is None else pre + part
        hidden[:, k * local : (k + 1) * local] = silu(pre + bias[k]).astype(BF)
    for r in range(QUARTERS):
        spot = far_spot(r, local)
        total = None
        for k in range(2):
            part = jnp.dot(hidden[:, k * local : (k + 1) * local], whole[k][1][:, spot], preferred_element_type=F32)
            behind = hidden[:, (k + 2) * local : (k + 3) * local]
            part += jnp.dot(behind, far[k][r][2 * local :, :], preferred_element_type=F32)
            total = part if total is None else total + part
        mixed_all[:, spot] = total
    live = lax.broadcasted_iota(jnp.int32, (rows, 1), 0) + first < count_ref[0]
    n_all[...] = finish(mixed_all[...], n_all[...].astype(F32), wide[:1, :], wide[1:2, :], live)
    for k in range(pairs):
        at = pl.ds(pl.multiple_of((me ^ k) * local, local), local)
        outs[k][...] = n_all[:, at]


def layer(
    node_latents,
    edge_latents,
    edge_sender,
    edge_receiver,
    block_owner,
    node_counts,
    halo_nodes,
    w_endpoints,
    w_edge_in,
    edge_bias,
    w_edge_out,
    edge_gain,
    edge_shift,
    w_node_in,
    node_bias,
    w_node_out,
    node_gain,
    node_shift,
):
    patches = lax.axis_size("patch")
    pairs = lax.axis_size("pair")
    me = lax.axis_index("pair")
    full, local = w_edge_in.shape
    node_total = node_latents.shape[0]
    edge_total = edge_latents.shape[0]
    blocks, tile = edge_sender.shape
    halo = halo_nodes.shape[2]
    mine = blocks // pairs
    rows = edge_total // pairs
    quarter = node_total // pairs
    if pairs != QUARTERS or patches % QUARTERS or mine % 2 or halo & (halo - 1):
        raise ValueError("unsupported mesh")
    by_swap = patches <= 8 and halo % LANES == 0
    direct = blocks == patches and mine == 2

    def to_pairs(pieces):
        far = {k: swap(pieces[k], "pair", k) for k in (2, 3, 1)}
        return [pieces[0]] + [far[k] for k in range(1, pairs)]

    send_list = halo_nodes[0]
    if by_swap:
        picked = halo_rows(True, send_list, node_latents)
        table = [picked[0]] + [swap(picked[k], "patch", k) for k in range(1, patches)]
    else:
        picked = halo_rows(False, send_list.reshape(-1, 2 * LANES), node_latents)
        table = [lax.all_to_all(jnp.concatenate(picked, axis=0), "patch", 0, 0, tiled=True)]

    w_nodes = w_node_in.reshape(2 * full, local)
    e_piece, n_piece = pl.pallas_call(
        functools.partial(pieces_kernel, local),
        in_specs=[HBM] * 5,
        out_specs=[VMEM] * 2,
        out_shape=[jax.ShapeDtypeStruct((4 * local, local), BF), jax.ShapeDtypeStruct((3 * local, local), BF)],
        scratch_shapes=[pltpu.VMEM((local, 2, local), BF), pltpu.SemaphoreType.DMA((6,))],
    )(w_edge_in, w_endpoints, w_edge_out, w_nodes, w_node_out)
    parted = pl.pallas_call(
        parted_kernel,
        compiler_params=grant(12),
        in_specs=[VMEM],
        out_specs=VMEM,
        out_shape=jax.ShapeDtypeStruct((2 * full, local), BF),
    )(w_endpoints)

    def gather_slices(own, piece, cut=None):
        parts = list(own) + [swap(w, "pair", 1) for w in own]
        near = swap(piece, "pair", 2)
        side = swap(near, "patch", 1)
        ahead = swap(near, "patch", 2)
        far = [near, side, ahead, swap(side if cut is None else side[:cut], "patch", 2)]
        if cut is not None:
            far.append(swap(ahead[cut:], "patch", 1))
        return parts + far + [swap(w, "pair", 1) for w in far]

    e_weights = gather_slices((w_edge_in, parted, w_edge_out), e_piece, 2 * local)
    n_weights = gather_slices((w_nodes, w_node_out), n_piece)

    e_parts = to_pairs(split(block_owner, tile, mine, direct, pairs, edge_latents, edge_bias, edge_gain, edge_shift))
    seen, segment, my_ids = sender_rows(by_swap, direct, pairs, halo, block_owner, edge_sender, edge_receiver, table)
    s_parts = to_pairs(seen)

    wide = full + LANES
    results = pl.pallas_call(
        functools.partial(edge_kernel, pairs, mine, direct),
        compiler_params=grant(28),
        in_specs=[SMEM] + [VMEM] * (2 + 2 * pairs + len(e_weights)),
        out_specs=[VMEM] * (pairs + mine),
        out_shape=[jax.ShapeDtypeStruct((rows, local), BF)] * pairs
        + [jax.ShapeDtypeStruct((RT, wide), BF)] * mine,
        scratch_shapes=[
            pltpu.VMEM((rows, full), BF),
            pltpu.VMEM((rows, full), BF),
            pltpu.VMEM((mine * RT, full), BF),
            pltpu.VMEM((rows, full), BF),
            pltpu.VMEM((rows, full), F32),
            pltpu.VMEM((rows, full), BF),
            pltpu.VMEM((8, full), F32),
        ],
        cost_estimate=pl.CostEstimate(
            flops=6 * rows * full * full, bytes_accessed=10 * full * full, transcendentals=rows * full
        ),
    )(
        block_owner,
        segment,
        my_ids,
        *e_parts,
        *s_parts,
        *e_weights,
    )
    new_edges, sums = results[:pairs], results[pairs:]

    if direct:
        got = []
        for t in range(mine):
            route = []
            for p in range(patches):
                for j in range(pairs):
                    to = (j * mine + (p % 2 ^ t)) * pairs + p // mine
                    route.append((p * pairs + j, to))
            got.append(lax.ppermute(sums[t], ("patch", "pair"), route))
        got = to_pairs([jnp.concatenate(got, axis=0)] * pairs)
    else:
        all_sums = jnp.stack(to_pairs([jnp.stack(sums)] * pairs)).reshape(blocks, RT * wide)
        peers = jnp.arange(pairs, dtype=jnp.int32) ^ me
        owners = block_owner.reshape(pairs, mine)[peers].reshape(-1)
        take = owners[None, :] == jnp.arange(patches, dtype=jnp.int32)[:, None]
        sent = jnp.dot(take.astype(BF), all_sums, preferred_element_type=F32).reshape(patches, RT, wide)
        none = jnp.any(take, axis=1)[:, None, None] | (jnp.arange(wide)[None, None, :] < full)
        sent = jnp.where(none, sent, -1.0).astype(BF)
        got = [lax.all_to_all(sent, "patch", 0, 0, tiled=True).reshape(patches * RT, wide)]

    new_edges = to_pairs(new_edges)
    edges_out = join(block_owner, tile, mine, direct, new_edges)

    n_parts = to_pairs(split(node_counts, quarter, 1, False, pairs, node_latents, node_bias, node_gain, node_shift))
    new_nodes = pl.pallas_call(
        functools.partial(node_kernel, pairs, len(got), direct),
        compiler_params=grant(20),
        in_specs=[SMEM] + [VMEM] * (1 + pairs + len(got) + len(n_weights)),
        out_specs=[VMEM] * pairs,
        out_shape=[jax.ShapeDtypeStruct((quarter, local), BF)] * pairs,
        scratch_shapes=[
            pltpu.VMEM((quarter, full), BF),
            pltpu.VMEM((patches * RT, full), BF),
            pltpu.VMEM((patches * RT, LANES), F32),
            pltpu.VMEM((quarter, full), BF),
            pltpu.VMEM((quarter, full), BF),
            pltpu.VMEM((quarter, full), F32),
            pltpu.VMEM((8, full), F32),
        ],
        cost_estimate=pl.CostEstimate(
            flops=6 * quarter * full * full, bytes_accessed=8 * full * full, transcendentals=quarter * full
        ),
    )(
        node_counts,
        send_list,
        *n_parts,
        *got,
        *n_weights,
    )
    nodes_out = join(node_counts, quarter, 1, False, to_pairs(new_nodes))
    return (nodes_out, edges_out)


def solution(mesh):
    return jax.shard_map(
        layer,
        mesh=mesh,
        in_specs=(
            P("patch", "pair"),
            P("patch", "pair"),
            P("patch", None),
            P("patch", None),
            P("patch"),
            P("patch"),
            P("patch", None, None),
            P(None, None, "pair"),
            P(None, "pair"),
            P("pair"),
            P("pair", None),
            P("pair"),
            P("pair"),
            P(None, None, "pair"),
            P("pair"),
            P("pair", None),
            P("pair"),
            P("pair"),
        ),
        out_specs=(P("patch", "pair"), P("patch", "pair")),
        check_vma=False,
    )
```
